32 devices in a mesh: wall: 8 (over y, x, core), span: 4 (over z).
Axes of the slice: x: 2, y: 2, z: 4, core: 2. Of those that a mesh axis runs over, the one named last changes fastest.
Arguments:
- velocity_old: float32 [3, 128, 64, 128], P(None, 'wall', 'span'), may hold values from -12 to 12, as said below
- heights: float32 [16], replicated, may hold values from 0.04 to 0.25
- owner_device: int32 [16384, 1], P(('wall', 'span')), may hold values from 0 to 7, as said below
- owner_element: int32 [16384, 1], P(('wall', 'span')), may hold values from 0 to 63, as said below
- ref_coords: float32 [3, 16384], P(None, ('wall', 'span')), may hold values from -1 to 1
- roughness: float32 [16384], P(('wall', 'span')), may hold values from 0.0001 to 0.01
Outputs:
- velocity_new: float32 [3, 128, 64, 128], P(None, 'wall', 'span')
- neumann: float32 [2, 16384], P(None, ('wall', 'span'))
The draws below stay inside these ranges and needn't reach their ends.
Inputs may be any that keep to these rules, and one draw needn't show every extreme that they name: `velocity_old`: values at coinciding nodes of neighbouring elements are equal. `owner_device`: the owner is the streamwise index w of the point's own device, or w + 1 or w - 1 modulo 8. Among the rows of one device at most 128 name w + 1 and at most 128 name w - 1; some device has exactly 128 for w + 1 and some device exactly 128 for w - 1. `owner_element`: the element index is (ex * 2 + ez) * 16 + ey with ex = i // 8 and ez = j // 8 of the wall point; ey < 2 for points of the first wall, ey >= 14 for the second.
All inputs are finite; a program needn't handle non-finite values.
Results may differ from the reference program's by a relative error of at most 0.0003.
Values sent between devices are 32-bit elements; how exact they have to be, the bound alone decides.
A program may use at most 128 MiB of HBM per device.

```python
import math
import jax
import jax.numpy as jnp
import numpy as np
from jax import lax

ORDER = 7
QN = 8
EXD = 2
EZD = 2
EY = 16
NEAR = 2
ITERS = 3
XLOC = 16
ZLOC = 16
YNODES = 128
XNODES = 128
ZNODES = 64
P_DEV = 512
WALLPTS = 16384
CAP = 128
N_WALL = 8
N_SPAN = 4
DEVICES = 32


def draw_velocity_old(key, part):
    unique_x = XNODES // QN * ORDER
    unique_z = ZNODES // QN * ORDER
    unique_y = EY * ORDER + 1
    index_x = (jnp.arange(XNODES) // QN * ORDER + jnp.arange(XNODES) % QN) % unique_x
    index_z = (jnp.arange(ZNODES) // QN * ORDER + jnp.arange(ZNODES) % QN) % unique_z
    index_y = jnp.arange(YNODES) // QN * ORDER + jnp.arange(YNODES) % QN
    shape_grid = (3, unique_x, unique_z, unique_y)
    values_grid = jax.random.truncated_normal(key, -4.0, 4.0, shape_grid, jnp.float32)
    rising = jnp.exp(jnp.log(3.0) * jnp.arange(unique_x, dtype=jnp.float32) / unique_x)
    values_grid = values_grid * rising[None, :, None, None]
    values_grid = jnp.take(values_grid, index_x, axis=1)
    values_grid = jnp.take(values_grid, index_z, axis=2)
    return jnp.take(values_grid, index_y, axis=3)


def draw_owner_device(key, part):
    block_keys = jax.random.split(jax.random.fold_in(key, 21), DEVICES)
    ranks = jax.vmap(lambda single: jax.random.permutation(single, P_DEV))(block_keys).astype(jnp.int32)
    blocks = jnp.arange(DEVICES, dtype=jnp.int32)
    count_next = jax.random.randint(jax.random.fold_in(key, 22), (DEVICES,), CAP // 3, CAP + 1)
    count_prev = jax.random.randint(jax.random.fold_in(key, 23), (DEVICES,), CAP // 3, CAP + 1)
    full_next = jax.random.randint(jax.random.fold_in(key, 24), (), 0, DEVICES)
    full_prev = jax.random.randint(jax.random.fold_in(key, 25), (), 0, DEVICES)
    count_next = jnp.where(blocks == full_next, CAP, count_next)
    count_prev = jnp.where(blocks == full_prev, CAP, count_prev)
    offset = jnp.where(ranks < count_next[:, None], 1, jnp.where(ranks < (count_next + count_prev)[:, None], -1, 0))
    own_wall = (blocks // N_SPAN)[:, None]
    owner = (own_wall + offset + N_WALL) % N_WALL
    return owner.astype(jnp.int32).reshape(WALLPTS, 1)


def draw_owner_element(key, part):
    position = jnp.arange(WALLPTS, dtype=jnp.int32) % P_DEV
    side_flag = position // (P_DEV // 2)
    node_i = position // ZLOC % XLOC
    node_j = position % ZLOC
    elem_x = node_i // QN
    elem_z = node_j // QN
    layer = jax.random.randint(jax.random.fold_in(key, 13), (WALLPTS,), 0, NEAR)
    elem_y = jnp.where(side_flag == 1, EY - 1 - layer, layer)
    return ((elem_x * EZD + elem_z) * EY + elem_y).astype(jnp.int32).reshape(WALLPTS, 1)


def levels(rng, shape, cuts, low, high):
    level = 1.0
    for axis_at, parts in cuts:
        steps = jax.random.uniform(jax.random.fold_in(jax.random.fold_in(rng, 6), axis_at), (parts,), jnp.float32, low / len(cuts), high / len(cuts))
        level = level * jnp.repeat(jnp.exp(steps), shape[axis_at] // parts).reshape((-1,) + (1,) * (len(shape) - 1 - axis_at))
    return level


def setup_inputs(seed: int = 0) -> dict:
    keys = jax.random.split(jax.random.key(seed), 7)
    return {
        "velocity_old": draw_velocity_old(jax.random.fold_in(keys[6], 71), 0),
        "heights": jnp.clip(jnp.exp(jax.random.uniform(keys[1], (EY,), jnp.float32, math.log(0.04), math.log(0.25))), 0.04, 0.25),
        "owner_device": draw_owner_device(jax.random.fold_in(keys[6], 71), 0),
        "owner_element": draw_owner_element(jax.random.fold_in(keys[6], 71), 0),
        "ref_coords": jnp.clip(jax.random.uniform(keys[4], (3, WALLPTS), jnp.float32, -1.0, 1.0) * levels(keys[4], (3, WALLPTS), ((1, 32),), -0.4, 0.0), -1.0, 1.0),
        "roughness": jnp.clip(jnp.exp(math.log(0.01) - 4.6051702 * jax.random.uniform(keys[5], (WALLPTS,), jnp.float32) ** levels(keys[5], (WALLPTS,), ((0, 32),), -0.2, 0.2)), 0.0001, 0.01),
    }


GLL_NODES = (-1.0, -0.8717401485096066, -0.5917001814331423, -0.2092992179024789, 0.2092992179024789, 0.5917001814331423, 0.8717401485096066, 1.0)
GLL_WEIGHTS = (0.03571428571428571, 0.2107042271435061, 0.3411226924835044, 0.4124587946587038, 0.4124587946587038, 0.3411226924835044, 0.2107042271435061, 0.03571428571428571)
viscosity = 0.02
inverse_step = 20.0
karman = 0.41
sample_height = 0.1
speed_floor = 0.01
element_dx = 0.05
element_dz = 0.13
precise = lax.Precision.HIGHEST

def stiffness_table():
    points = np.array(GLL_NODES)
    weights = np.array(GLL_WEIGHTS)
    previous = np.ones(8)
    current = points.copy()
    for degree in range(1, 7):
        previous, current = (current, ((2 * degree + 1) * points * current - degree * previous) / (degree + 1))
    derivative = np.zeros((8, 8))
    for target in range(8):
        for source in range(8):
            if target != source:
                derivative[target, source] = current[target] / current[source] / (points[target] - points[source])
    derivative[0, 0] = -14.0
    derivative[7, 7] = 14.0
    return derivative.T @ (weights[:, None] * derivative)

def lagrange(coord):
    points = np.array(GLL_NODES)
    gaps_table = points[:, None] - points[None, :] + np.eye(8)
    scale_row = jnp.asarray(1.0 / np.prod(gaps_table, axis=1), jnp.float32)
    gaps = coord[:, None] - jnp.asarray(points, jnp.float32)[None, :]
    filled = jnp.where(jnp.asarray(np.eye(8) > 0.5)[None], jnp.float32(1.0), gaps[:, None, :])
    return jnp.prod(filled, axis=2) * scale_row[None, :]

def face_weights(length, open_ends):
    values = np.ones(length)
    position = np.arange(length) % 8
    values[(position == 0) | (position == 7)] = 0.5
    if open_ends:
        values[0] = 1.0
        values[-1] = 1.0
    return values

def join_faces(core, before, after, axis):
    count = core.shape[axis] // 8
    blocks = core.reshape(core.shape[:axis] + (count, 8) + core.shape[axis + 1:])
    first = lax.slice_in_dim(blocks, 0, 1, axis=axis + 1)
    last = lax.slice_in_dim(blocks, 7, 8, axis=axis + 1)
    before_b = jnp.expand_dims(before, axis + 1)
    after_b = jnp.expand_dims(after, axis + 1)
    prev_last = jnp.concatenate([before_b, lax.slice_in_dim(last, 0, count - 1, axis=axis)], axis)
    next_first = jnp.concatenate([lax.slice_in_dim(first, 1, count, axis=axis), after_b], axis)
    middle = lax.slice_in_dim(blocks, 1, 7, axis=axis + 1)
    joined = jnp.concatenate([first + prev_last, middle, last + next_first], axis + 1)
    return joined.reshape(core.shape)

def assemble(field):
    joined_x = join_faces(field, field[:, -1:], field[:, :1], 1)
    joined_z = join_faces(joined_x, joined_x[:, :, -1:], joined_x[:, :, :1], 2)
    border = jnp.zeros(joined_z.shape[:3] + (1,), jnp.float32)
    return join_faces(joined_z, border, border, 3)

def reference(velocity_old, heights, owner_device, owner_element, ref_coords, roughness):
    weights = np.array(GLL_WEIGHTS)
    stiffness = jnp.asarray(stiffness_table(), jnp.float32)
    length_x, length_z, length_y = (velocity_old.shape[1], velocity_old.shape[2], velocity_old.shape[3])
    count_x, count_z, count_y = (length_x // 8, length_z // 8, length_y // 8)
    mass_x = jnp.asarray(np.tile(0.5 * element_dx * weights, count_x), jnp.float32)
    mass_z = jnp.asarray(np.tile(0.5 * element_dz * weights, count_z), jnp.float32)
    mass_y = (0.5 * heights[:, None] * jnp.asarray(weights, jnp.float32)[None, :]).reshape(length_y)
    mass_all = mass_x[:, None, None] * mass_z[None, :, None] * mass_y[None, None, :]
    inverse_count = jnp.asarray(face_weights(length_x, False)[:, None, None] * face_weights(length_z, False)[None, :, None] * face_weights(length_y, True)[None, None, :], jnp.float32)
    blocks = (2.0 / heights)[:, None, None] * stiffness[None]

    def operate(field):
        along_x = jnp.einsum('ab,cebzy->ceazy', stiffness * (2.0 / element_dx), field.reshape(3, count_x, 8, length_z, length_y), precision=precise).reshape(field.shape)
        along_z = jnp.einsum('ab,cxeby->cxeay', stiffness * (2.0 / element_dz), field.reshape(3, length_x, count_z, 8, length_y), precision=precise).reshape(field.shape)
        along_y = jnp.einsum('eab,cxzeb->cxzea', blocks, field.reshape(3, length_x, length_z, count_y, 8), precision=precise).reshape(field.shape)
        mass_xb = mass_x[None, :, None, None]
        mass_zb = mass_z[None, None, :, None]
        mass_yb = mass_y[None, None, None, :]
        local = viscosity * (along_x * mass_zb * mass_yb + mass_xb * along_z * mass_yb + mass_xb * mass_zb * along_y) + inverse_step * mass_all[None] * field
        return assemble(local)
    element_rows = velocity_old.reshape(3, count_x, 8, count_z, 8, count_y, 8).transpose(1, 3, 5, 0, 2, 4, 6).reshape(count_x * count_z * count_y, 3 * 512)
    points = jnp.arange(WALLPTS, dtype=jnp.int32)
    span_index = points // P_DEV % N_SPAN
    local_elem = owner_element[:, 0]
    elem_x = owner_device[:, 0] * EXD + local_elem // (EZD * EY)
    elem_z = span_index * EZD + local_elem // EY % EZD
    elem_y = local_elem % EY
    row_ids = ((elem_x * count_z + elem_z) * count_y + elem_y).astype(jnp.int32)

    def evaluate(pieces):
        rows_here, coords = pieces
        values = element_rows[rows_here].reshape(rows_here.shape[0], 3, 8, 8, 8)
        return jnp.einsum('gcabd,ga,gb,gd->gc', values, lagrange(coords[:, 0]), lagrange(coords[:, 1]), lagrange(coords[:, 2]), precision=precise)
    sampled = lax.map(evaluate, (row_ids.reshape(DEVICES, P_DEV), ref_coords.T.reshape(DEVICES, P_DEV, 3))).reshape(WALLPTS, 3)
    stream = sampled[:, 0]
    spanwise = sampled[:, 2]
    wall_speed = jnp.sqrt(stream * stream + spanwise * spanwise + speed_floor)
    drag_coeff = (karman / jnp.log(sample_height / roughness)) ** 2
    neumann = -(drag_coeff * wall_speed / viscosity)[None, :] * jnp.stack([stream, spanwise])
    traction = (viscosity * neumann).reshape(2, N_WALL, N_SPAN, 2, XLOC, ZLOC).transpose(0, 3, 1, 4, 2, 5).reshape(2, 2, length_x, length_z)
    traction = traction * (mass_x[:, None] * mass_z[None, :])[None, None]
    zero_plane = jnp.zeros((1, length_x, length_z), jnp.float32)
    bottom = jnp.concatenate([traction[0:1, 0], zero_plane, traction[1:2, 0]], axis=0)
    top_wall = jnp.concatenate([traction[0:1, 1], zero_plane, traction[1:2, 1]], axis=0)
    forcing = inverse_step * mass_all[None] * velocity_old
    forcing = forcing.at[:, :, :, 0].add(bottom).at[:, :, :, -1].add(top_wall)
    right_side = assemble(forcing)

    def weighted(first, second):
        return lax.optimization_barrier(jnp.sum(first * second * inverse_count[None], axis=(1, 2, 3)))

    def spread(values):
        return values[:, None, None, None]
    solution = jnp.zeros_like(right_side)
    residual = right_side
    direction = residual
    norm_now = weighted(residual, residual)
    for sweep in range(ITERS):
        applied = operate(direction)
        step_size = norm_now / weighted(direction, applied)
        solution = solution + spread(step_size) * direction
        residual = residual - spread(step_size) * applied
        norm_next = weighted(residual, residual)
        direction = residual + spread(norm_next / norm_now) * direction
        norm_now = norm_next
    return (solution, neumann)
```

```python
import functools

import jax
import jax.numpy as jnp
import numpy as np
from jax import lax
from jax.experimental import pallas as pl
from jax.experimental.pallas import tpu as pltpu
from jax.sharding import PartitionSpec as P

GLL_NODES = (
    -1.0,
    -0.8717401485096066,
    -0.5917001814331423,
    -0.2092992179024789,
    0.2092992179024789,
    0.5917001814331423,
    0.8717401485096066,
    1.0,
)
GLL_WEIGHTS = (
    0.03571428571428571,
    0.2107042271435061,
    0.3411226924835044,
    0.4124587946587038,
    0.4124587946587038,
    0.3411226924835044,
    0.2107042271435061,
    0.03571428571428571,
)
viscosity = 0.02
inverse_step = 20.0
karman = 0.41
sample_height = 0.1
speed_floor = 0.01
element_dx = 0.05
element_dz = 0.13
NEAR = 2
ROUNDS = 3
MESH = pl.DeviceIdType.MESH
F32 = jnp.float32
BF16 = jnp.bfloat16


def stiffness_table():
    points = np.array(GLL_NODES)
    weights = np.array(GLL_WEIGHTS)
    previous = np.ones(8)
    current = points.copy()
    for degree in range(1, 7):
        previous, current = (
            current,
            ((2 * degree + 1) * points * current - degree * previous) / (degree + 1),
        )
    derivative = np.zeros((8, 8))
    for target in range(8):
        for source in range(8):
            if target != source:
                derivative[target, source] = (
                    current[target] / current[source] / (points[target] - points[source])
                )
    derivative[0, 0] = -14.0
    derivative[7, 7] = 14.0
    return derivative.T @ (weights[:, None] * derivative)


def join_matrix(length):
    joined = np.eye(length)
    for left in range(7, length - 1, 8):
        joined[left, left + 1] = 1.0
        joined[left + 1, left] = 1.0
    return joined


def face_weights(length, open_ends):
    values = np.ones(length)
    position = np.arange(length) % 8
    values[(position == 0) | (position == 7)] = 0.5
    if open_ends:
        values[0] = 1.0
        values[-1] = 1.0
    return values


def split_np(matrix):
    single = jnp.asarray(matrix, F32)
    high = single.astype(BF16)
    low = (jnp.asarray(matrix, F32) - high.astype(F32)).astype(BF16)
    return high, low


def tables(length_x, length_z, length_y):
    weights = np.array(GLL_WEIGHTS)
    stiffness = stiffness_table()
    count_x, count_z, count_y = length_x // 8, length_z // 8, length_y // 8
    mass_x = np.tile(0.5 * element_dx * weights, count_x)
    mass_z = np.tile(0.5 * element_dz * weights, count_z)
    stiff_x = np.kron(np.eye(count_x), stiffness * (2.0 / element_dx))
    stiff_z = np.kron(np.eye(count_z), stiffness * (2.0 / element_dz))
    mass_xz = np.kron(mass_x, mass_z)
    join_xz = np.kron(join_matrix(length_x), join_matrix(length_z))
    join_y = join_matrix(length_y)
    plane = viscosity * (
        np.kron(stiff_x, np.diag(mass_z)) + np.kron(np.diag(mass_x), stiff_z)
    ) + inverse_step * np.diag(mass_xz)
    plane = join_xz @ plane
    mass_plane = join_xz @ np.diag(mass_xz)
    both = np.concatenate([plane, mass_plane], axis=1)
    lines_mass = np.tile(0.5 * weights, count_y)[:, None] * join_y
    lines_stiff = viscosity * 2.0 * (np.kron(np.eye(count_y), stiffness) @ join_y)
    lines = np.stack([lines_mass, lines_stiff])
    full = np.tile(mass_x, 3)
    ring_x = join_matrix(length_x) @ mass_x
    ring_z = join_matrix(length_z) @ mass_z
    ring_x[0] *= 2.0
    ring_x[-1] *= 2.0
    ring_z[0] *= 2.0
    ring_z[-1] *= 2.0
    del full
    assembled = inverse_step * np.kron(ring_x, ring_z)
    inner_x = face_weights(length_x, True)
    inner_z = face_weights(length_z, True)
    outer_x = face_weights(length_x, False)
    outer_z = face_weights(length_z, False)
    weight_y = face_weights(length_y, True)
    columns = np.stack(
        [
            assembled[:, None] * np.ones(length_y)[None],
            np.kron(outer_x, outer_z)[:, None] * weight_y[None],
            np.kron(inner_x, inner_z)[:, None] * weight_y[None],
        ]
    )
    return both, lines, columns


def split(value):
    high = value.astype(BF16)
    low = (value - high.astype(F32)).astype(BF16)
    return high, low


def dot3(left, right, dims):
    def one(a, b):
        return lax.dot_general(a, b, (dims, ((), ())), preferred_element_type=F32)

    return one(left[0], right[0]) + (one(left[0], right[1]) + one(left[1], right[0]))


NN = ((1,), (0,))
NT = ((1,), (1,))
TN = ((0,), (0,))
DIRS = ((1, 1), (1, -1), (-1, 1), (-1, -1))


def lagrange_rows(coord):
    points = np.array(GLL_NODES)
    scale = 1.0 / np.prod(points[:, None] - points[None, :] + np.eye(8), axis=1)
    shape = (8, coord.shape[1])
    node = lax.broadcasted_iota(jnp.int32, shape, 0)
    total = jnp.zeros(shape, F32)
    for a in range(8):
        total = jnp.where(node == a, F32(scale[a]), total)
    for b in range(8):
        total = total * jnp.where(node == b, F32(1.0), coord - F32(points[b]))
    return total


def kernel(
    n_wall,
    n_span,
    sizes,
    vel,
    heights,
    owner,
    element,
    coords,
    roughness,
    plane_hi,
    plane_lo,
    lines,
    columns,
    out,
    neumann,
    near,
    near_got,
    field,
    local,
    z_send,
    c_send,
    x_got,
    z_got,
    c_got,
    parts,
    sum_send,
    wall_got,
    span_got,
    near_ss,
    near_rs,
    face_ss,
    face_rs,
    wall_ss,
    wall_rs,
    span_ss,
    span_rs,
):
    length_x, length_z, length_y = sizes
    rows = length_x * length_z
    count_z, count_y = length_z // 8, length_y // 8
    w = lax.axis_index("wall")
    s = lax.axis_index("span")

    def at(dx, dz):
        return (lax.rem(w + (dx + n_wall), n_wall), lax.rem(s + (dz + n_span), n_span))

    greeted = [(k, 0) for k in range(1, n_wall)] + [(0, k) for k in range(1, n_span)]
    greeted += list(DIRS)
    barrier = pltpu.get_barrier_semaphore()
    for dx, dz in greeted:
        pl.semaphore_signal(barrier, inc=1, device_id=at(dx, dz), device_id_type=MESH)

    lane = lax.broadcasted_iota(jnp.int32, (64, length_y), 1)
    groups = (length_x // 8) * count_z
    for index, comp in enumerate((0, 2)):
        packed = jnp.zeros((64, length_y), F32)
        for group in range(groups):
            ex, ez = group // count_z, group % count_z
            block = vel[comp, pl.ds(ex * 8, 8), pl.ds(ez * 8, 8), :].reshape(64, length_y)
            moved = pltpu.roll(block, (group * 32 + 16) % length_y, 1)
            packed = jnp.where(lane // 32 == group, moved, packed)
        near[index] = packed
    pl.semaphore_wait(barrier, len(greeted))

    def remote(src, dst, ss, rs, where):
        return pltpu.make_async_remote_copy(
            src_ref=src,
            dst_ref=dst,
            send_sem=ss,
            recv_sem=rs,
            device_id=where,
            device_id_type=MESH,
        )

    near_copies = []
    for slot, dx in enumerate((1, -1)):
        copy = remote(near, near_got.at[slot], near_ss.at[slot], near_rs.at[slot], at(dx, 0))
        copy.start()
        near_copies.append(copy)

    layer_of = lax.broadcasted_iota(jnp.int32, (length_y, count_y), 0) // 8
    layer = lax.broadcasted_iota(jnp.int32, (length_y, count_y), 1)
    height_row = heights[...]
    height = jnp.sum(jnp.where(layer_of == layer, height_row, 0.0), axis=1, keepdims=True)
    lines_mass = height * lines[0]
    lines_hi, lines_lo = split(jnp.concatenate([lines_mass, lines[1] / height], axis=1))
    bound = jnp.max(0.1535 * height_row + 0.000182 / height_row, axis=1, keepdims=True)
    shifts = (0.15 * bound, 0.85 * bound)

    mass_row = jnp.sum(lines_mass, axis=0, keepdims=True)
    scale = columns[0] * mass_row
    for c in range(3):
        field[0, c] = vel[c].reshape(rows, length_y) * scale

    points = owner.shape[1]
    row_x = lagrange_rows(coords[0:1, :])
    row_z = lagrange_rows(coords[1:2, :])
    row_y = lagrange_rows(coords[2:3, :])
    cross = jnp.concatenate([row_x[a : a + 1] * row_z for a in range(8)], axis=0)
    distance = lax.rem(owner[...] - w + n_wall, n_wall)
    from_next = distance == 1
    from_prev = distance == n_wall - 1
    own = jnp.logical_not(jnp.logical_or(from_next, from_prev))
    spread = jnp.concatenate(
        [jnp.where(mask, cross, 0.0) for mask in (own, from_prev, from_next)], axis=0
    )
    n_row = lax.broadcasted_iota(jnp.int32, (length_y, points), 0)
    within = (n_row % 32) // 8
    layer_y = jnp.where(within < NEAR, within + (count_y - NEAR), within - NEAR)
    wanted = (n_row // 32) * count_y + layer_y == element[...]
    along = jnp.where(wanted, jnp.concatenate([row_y] * (length_y // 8), axis=0), 0.0)
    spread = split(spread)

    for copy in near_copies:
        copy.wait()

    sampled = []
    for index in range(2):
        sources = jnp.concatenate(
            [near[index], near_got[0, index], near_got[1, index]], axis=0
        )
        values = dot3(split(sources), spread, TN)
        sampled.append(jnp.sum(values * along, axis=0, keepdims=True))
    stream, spanwise = sampled
    speed = jnp.sqrt(stream * stream + spanwise * spanwise + speed_floor)
    drag = karman / jnp.log(sample_height / roughness[...])
    factor = -(drag * drag * speed / viscosity)
    gradient = (factor * stream, factor * spanwise)
    neumann[0:1, :] = gradient[0]
    neumann[1:2, :] = gradient[1]

    def face_copies(turn):
        copies = []
        for slot, dx in enumerate((1, -1)):
            start = rows - length_z if dx == 1 else 0
            copies.append(
                remote(
                    local.at[turn, :, pl.ds(start, length_z), :],
                    x_got.at[turn, slot],
                    face_ss.at[turn, slot],
                    face_rs.at[turn, slot],
                    at(dx, 0),
                )
            )
        for slot, dz in enumerate((1, -1)):
            copies.append(
                remote(
                    z_send.at[turn, slot],
                    z_got.at[turn, slot],
                    face_ss.at[turn, 2 + slot],
                    face_rs.at[turn, 2 + slot],
                    at(0, dz),
                )
            )
        for slot, (dx, dz) in enumerate(DIRS):
            copies.append(
                remote(
                    c_send.at[turn, slot],
                    c_got.at[turn, slot],
                    face_ss.at[turn, 4 + slot],
                    face_rs.at[turn, 4 + slot],
                    at(dx, dz),
                )
            )
        return copies

    def corner(dx, dz):
        return (rows - length_z if dx == 1 else 0) + (length_z - 1 if dz == 1 else 0)

    def send_faces(turn):
        for c in range(3):
            for slot, dz in enumerate((1, -1)):
                edge = length_z - 1 if dz == 1 else 0
                z_send[turn, slot, c] = local[turn, c, pl.ds(edge, length_x, stride=length_z), :]
            for slot, (dx, dz) in enumerate(DIRS):
                at_row = corner(dx, dz)
                c_send[turn, slot, c : c + 1, :] = local[turn, c, at_row : at_row + 1, :]
        for slot in range(4):
            c_send[turn, slot, 3:8, :] = jnp.zeros((5, length_y), F32)
        copies = face_copies(turn)
        for copy in copies:
            copy.start()
        return copies

    def add_faces(turn, copies):
        for copy in copies:
            copy.wait()
        for c in range(3):
            for slot, dx in enumerate((1, -1)):
                start = 0 if dx == 1 else rows - length_z
                field[turn, c, pl.ds(start, length_z), :] += x_got[turn, slot, c]
            for slot, dz in enumerate((1, -1)):
                edge = pl.ds(0 if dz == 1 else length_z - 1, length_x, stride=length_z)
                field[turn, c, edge, :] = field[turn, c, edge, :] + z_got[turn, slot, c]
            for slot, (dx, dz) in enumerate(DIRS):
                at_row = corner(-dx, -dz)
                field[turn, c, at_row : at_row + 1, :] += c_got[turn, slot, c : c + 1, :]

    def inner(quantity, c, product):
        parts[quantity * 8 + c : quantity * 8 + c + 1, :] = jnp.sum(
            product, axis=0, keepdims=True
        )

    n_line = lax.broadcasted_iota(jnp.int32, (length_y, rows), 0)
    mass_hi = plane_hi[:, rows:]
    mass_lo = plane_lo[:, rows:]
    for index, c in enumerate((0, 2)):
        pull = viscosity * gradient[index]
        lifted = jnp.where(
            n_line == 0, pull[:, :rows], jnp.where(n_line == length_y - 1, pull[:, rows:], 0.0)
        )
        local[0, c] = dot3((mass_hi, mass_lo), split(lifted), NT)
    local[0, 1] = jnp.zeros((rows, length_y), F32)
    copies = send_faces(0)
    parts[...] = jnp.zeros_like(parts)
    for c in (0, 2):
        field[0, c] += local[0, c]
    add_faces(0, copies)

    def operate(source, target):
        for c in range(3):
            lined = dot3(split(field[source, c]), (lines_hi, lines_lo), NN)
            stacked = jnp.concatenate([lined[:, :length_y], lined[:, length_y:]], axis=0)
            local[target, c] = dot3((plane_hi[...], plane_lo[...]), split(stacked), NN)

    slots = {(0, 0): 0, (0, 1): 1, (1, 1): 2, (0, 2): 3, (1, 2): 4, (2, 2): 5}

    def inner_products(newest):
        for c in range(3):
            weighted = field[newest, c] * columns[1]
            for other in range(newest + 1):
                inner(slots[(other, newest)], c, weighted * field[other, c])

    for turn in (1, 2):
        operate(turn - 1, turn)
        copies = send_faces(turn)
        for c in range(3):
            field[turn, c] = local[turn, c] - shifts[turn - 1] * field[turn - 1, c]
        inner_products(turn - 1)
        add_faces(turn, copies)
    operate(2, 3)
    inner_products(2)
    for c in range(3):
        inner(6, c, field[2, c] * columns[2] * local[3, c])

    total_rows = parts.shape[0]
    r_iota = lax.broadcasted_iota(jnp.int32, (total_rows, 128), 0)
    l_iota = lax.broadcasted_iota(jnp.int32, (total_rows, 128), 1)
    diagonal = r_iota == l_iota
    summed = jnp.sum(parts[...], axis=1, keepdims=True)
    row = jnp.sum(jnp.where(diagonal, summed, 0.0), axis=0, keepdims=True)

    def gather_sum(stage, row, count, got, ss, rs, place):
        sum_send[stage] = jnp.broadcast_to(row, (8, 128))
        copies = []
        for k in range(1, count):
            copy = remote(
                sum_send.at[stage], got.at[k - 1], ss.at[k - 1], rs.at[k - 1], place(k)
            )
            copy.start()
            copies.append(copy)
        for copy in copies:
            copy.wait()
        total = row
        for k in range(1, count):
            total = total + got[k - 1, 0:1, :]
        return total

    row = gather_sum(0, row, n_wall, wall_got, wall_ss, wall_rs, lambda k: at(k, 0))
    row = gather_sum(1, row, n_span, span_got, span_ss, span_rs, lambda k: at(0, k))
    totals = jnp.sum(jnp.where(diagonal, row, 0.0), axis=1, keepdims=True)
    m00, m01, m11, m02, m12, m22, e22 = [totals[q * 8 : q * 8 + 8, :] for q in range(7)]
    t1, t2 = shifts
    a00 = m01 + t1 * m00
    a01 = m11 + t1 * m01
    a02 = m12 + t1 * m02
    a11 = m12 + t2 * m11
    a12 = m22 + t2 * m12
    l10 = a01 / a00
    l20 = a02 / a00
    d1 = a11 - l10 * a01
    u12 = a12 - l10 * a02
    l21 = u12 / d1
    d2 = e22 - l20 * a02 - l21 * u12
    y1 = m01 - l10 * m00
    y2 = m02 - l20 * m00 - l21 * y1
    x2 = y2 / d2
    x1 = y1 / d1 - l21 * x2
    x0 = m00 / a00 - l10 * x1 - l20 * x2
    for c in range(3):
        result = (
            x0[c : c + 1] * field[0, c] + x1[c : c + 1] * field[1, c] + x2[c : c + 1] * field[2, c]
        )
        out[c] = result.reshape(length_x, length_z, length_y)


def body(n_wall, n_span, velocity_old, heights, owner_device, owner_element, ref_coords, roughness):
    sizes = velocity_old.shape[1:]
    length_x, length_z, length_y = sizes
    rows = length_x * length_z
    points = owner_device.shape[0]
    both, lines, columns = tables(*sizes)
    plane_hi, plane_lo = split_np(both)
    vmem = pl.BlockSpec(memory_space=pltpu.VMEM)
    dma = pltpu.SemaphoreType.DMA
    return pl.pallas_call(
        functools.partial(kernel, n_wall, n_span, sizes),
        out_shape=(
            jax.ShapeDtypeStruct(velocity_old.shape, F32),
            jax.ShapeDtypeStruct((2, points), F32),
        ),
        in_specs=[vmem] * 10,
        out_specs=(vmem, vmem),
        scratch_shapes=[
            pltpu.VMEM((2, 64, length_y), F32),
            pltpu.VMEM((2, 2, 64, length_y), F32),
            pltpu.VMEM((3, 3, rows, length_y), F32),
            pltpu.VMEM((4, 3, rows, length_y), F32),
            pltpu.VMEM((ROUNDS, 2, 3, length_x, length_y), F32),
            pltpu.VMEM((ROUNDS, 4, 8, length_y), F32),
            pltpu.VMEM((ROUNDS, 2, 3, length_z, length_y), F32),
            pltpu.VMEM((ROUNDS, 2, 3, length_x, length_y), F32),
            pltpu.VMEM((ROUNDS, 4, 8, length_y), F32),
            pltpu.VMEM((56, length_y), F32),
            pltpu.VMEM((2, 8, 128), F32),
            pltpu.VMEM((n_wall - 1, 8, 128), F32),
            pltpu.VMEM((n_span - 1, 8, 128), F32),
            dma((2,)),
            dma((2,)),
            dma((ROUNDS, 8)),
            dma((ROUNDS, 8)),
            dma((n_wall - 1,)),
            dma((n_wall - 1,)),
            dma((n_span - 1,)),
            dma((n_span - 1,)),
        ],
        compiler_params=pltpu.CompilerParams(
            collective_id=0, has_side_effects=True, vmem_limit_bytes=48 * 1024 * 1024
        ),
    )(
        velocity_old,
        heights.reshape(1, -1),
        owner_device.reshape(1, -1),
        owner_element.reshape(1, -1),
        ref_coords,
        roughness.reshape(1, -1),
        plane_hi,
        plane_lo,
        jnp.asarray(lines, F32),
        jnp.asarray(columns, F32),
    )


def solution(mesh):
    placed = (
        P(None, "wall", "span", None),
        P(),
        P(("wall", "span"), None),
        P(("wall", "span"), None),
        P(None, ("wall", "span")),
        P(("wall", "span")),
    )
    return jax.shard_map(
        functools.partial(body, mesh.shape["wall"], mesh.shape["span"]),
        mesh=mesh,
        in_specs=placed,
        out_specs=(P(None, "wall", "span", None), P(None, ("wall", "span"))),
        check_vma=False,
    )
```

```python
import functools

import jax
import jax.numpy as jnp
import numpy as np
from jax import lax
from jax.experimental import pallas as pl
from jax.experimental.pallas import tpu as pltpu
from jax.sharding import PartitionSpec as P

GLL_NODES = (
    -1.0,
    -0.8717401485096066,
    -0.5917001814331423,
    -0.2092992179024789,
    0.2092992179024789,
    0.5917001814331423,
    0.8717401485096066,
    1.0,
)
GLL_WEIGHTS = (
    0.03571428571428571,
    0.2107042271435061,
    0.3411226924835044,
    0.4124587946587038,
    0.4124587946587038,
    0.3411226924835044,
    0.2107042271435061,
    0.03571428571428571,
)
viscosity = 0.02
inverse_step = 20.0
karman = 0.41
sample_height = 0.1
speed_floor = 0.01
element_dx = 0.05
element_dz = 0.13
NEAR = 2
ROUNDS = 3
SINGLE_STAGE = 64
MESH = pl.DeviceIdType.MESH
F32 = jnp.float32
BF16 = jnp.bfloat16


def stiffness_table():
    points = np.array(GLL_NODES)
    weights = np.array(GLL_WEIGHTS)
    previous = np.ones(8)
    current = points.copy()
    for degree in range(1, 7):
        previous, current = (
            current,
            ((2 * degree + 1) * points * current - degree * previous) / (degree + 1),
        )
    derivative = np.zeros((8, 8))
    for target in range(8):
        for source in range(8):
            if target != source:
                derivative[target, source] = (
                    current[target] / current[source] / (points[target] - points[source])
                )
    derivative[0, 0] = -14.0
    derivative[7, 7] = 14.0
    return derivative.T @ (weights[:, None] * derivative)


def join_matrix(length):
    joined = np.eye(length)
    for left in range(7, length - 1, 8):
        joined[left, left + 1] = 1.0
        joined[left + 1, left] = 1.0
    return joined


def face_weights(length, open_ends):
    values = np.ones(length)
    position = np.arange(length) % 8
    values[(position == 0) | (position == 7)] = 0.5
    if open_ends:
        values[0] = 1.0
        values[-1] = 1.0
    return values


def split_np(matrix):
    single = jnp.asarray(matrix, F32)
    high = single.astype(BF16)
    low = (jnp.asarray(matrix, F32) - high.astype(F32)).astype(BF16)
    return high, low


def tables(length_x, length_z, length_y):
    weights = np.array(GLL_WEIGHTS)
    stiffness = stiffness_table()
    count_x, count_z, count_y = length_x // 8, length_z // 8, length_y // 8
    mass_x = np.tile(0.5 * element_dx * weights, count_x)
    mass_z = np.tile(0.5 * element_dz * weights, count_z)
    stiff_x = np.kron(np.eye(count_x), stiffness * (2.0 / element_dx))
    stiff_z = np.kron(np.eye(count_z), stiffness * (2.0 / element_dz))
    mass_xz = np.kron(mass_x, mass_z)
    join_xz = np.kron(join_matrix(length_x), join_matrix(length_z))
    join_y = join_matrix(length_y)
    plane = viscosity * (
        np.kron(stiff_x, np.diag(mass_z)) + np.kron(np.diag(mass_x), stiff_z)
    ) + inverse_step * np.diag(mass_xz)
    plane = join_xz @ plane
    mass_plane = join_xz @ np.diag(mass_xz)
    both = np.concatenate([plane, mass_plane], axis=1)
    lines_mass = np.tile(0.5 * weights, count_y)[:, None] * join_y
    lines_stiff = viscosity * 2.0 * (np.kron(np.eye(count_y), stiffness) @ join_y)
    lines = np.stack([lines_mass, lines_stiff])
    full = np.tile(mass_x, 3)
    ring_x = join_matrix(length_x) @ mass_x
    ring_z = join_matrix(length_z) @ mass_z
    ring_x[0] *= 2.0
    ring_x[-1] *= 2.0
    ring_z[0] *= 2.0
    ring_z[-1] *= 2.0
    del full
    assembled = inverse_step * np.kron(ring_x, ring_z)
    inner_x = face_weights(length_x, True)
    inner_z = face_weights(length_z, True)
    outer_x = face_weights(length_x, False)
    outer_z = face_weights(length_z, False)
    weight_y = face_weights(length_y, True)
    columns = np.stack(
        [
            assembled[:, None] * np.ones(length_y)[None],
            np.kron(outer_x, outer_z)[:, None] * weight_y[None],
            np.kron(inner_x, inner_z)[:, None] * weight_y[None],
        ]
    )
    return both, lines, columns


def split(value):
    high = value.astype(BF16)
    low = (value - high.astype(F32)).astype(BF16)
    return high, low


def dot3(left, right, dims):
    def one(a, b):
        return lax.dot_general(a, b, (dims, ((), ())), preferred_element_type=F32)

    return one(left[0], right[0]) + (one(left[0], right[1]) + one(left[1], right[0]))


NN = ((1,), (0,))
NT = ((1,), (1,))
TN = ((0,), (0,))
DIRS = ((1, 1), (1, -1), (-1, 1), (-1, -1))


def lagrange_rows(coord):
    points = np.array(GLL_NODES)
    scale = 1.0 / np.prod(points[:, None] - points[None, :] + np.eye(8), axis=1)
    shape = (8, coord.shape[1])
    node = lax.broadcasted_iota(jnp.int32, shape, 0)
    total = jnp.zeros(shape, F32)
    for a in range(8):
        total = jnp.where(node == a, F32(scale[a]), total)
    for b in range(8):
        total = total * jnp.where(node == b, F32(1.0), coord - F32(points[b]))
    return total


def kernel(
    n_wall,
    n_span,
    sizes,
    vel_in,
    heights_in,
    owner_in,
    element_in,
    coords_in,
    roughness_in,
    plane_hi_in,
    plane_lo_in,
    lines_in,
    columns_in,
    out,
    neumann,
    vel,
    heights,
    owner,
    element,
    coords,
    roughness,
    plane_hi,
    plane_lo,
    lines,
    columns,
    load_sem,
    near,
    near_got,
    field,
    local,
    z_send,
    c_send,
    x_got,
    z_got,
    c_got,
    parts,
    sum_send,
    wall_got,
    span_got,
    near_ss,
    near_rs,
    face_ss,
    face_rs,
    wall_ss,
    wall_rs,
    span_ss,
    span_rs,
):
    length_x, length_z, length_y = sizes
    rows = length_x * length_z
    count_z, count_y = length_z // 8, length_y // 8
    w = lax.axis_index("wall")
    s = lax.axis_index("span")

    def at(dx, dz):
        return (lax.rem(w + (dx + n_wall), n_wall), lax.rem(s + (dz + n_span), n_span))

    loads = [
        pltpu.make_async_copy(source, target, load_sem.at[index])
        for index, (source, target) in enumerate(
            (
                (vel_in, vel),
                (heights_in, heights),
                (lines_in, lines),
                (coords_in, coords),
                (owner_in, owner),
                (element_in, element),
                (columns_in, columns),
                (roughness_in, roughness),
                (plane_hi_in, plane_hi),
                (plane_lo_in, plane_lo),
            )
        )
    ]
    for load in loads:
        load.start()

    single = n_wall * n_span <= SINGLE_STAGE
    if single:
        greeted = [divmod(k, n_span) for k in range(1, n_wall * n_span)]
    else:
        greeted = [(k, 0) for k in range(1, n_wall)] + [(0, k) for k in range(1, n_span)]
        greeted += list(DIRS)
    barrier = pltpu.get_barrier_semaphore()
    for dx, dz in greeted:
        pl.semaphore_signal(barrier, inc=1, device_id=at(dx, dz), device_id_type=MESH)

    loads[0].wait()
    lane = lax.broadcasted_iota(jnp.int32, (64, length_y), 1)
    groups = (length_x // 8) * count_z
    for index, comp in enumerate((0, 2)):
        packed = jnp.zeros((64, length_y), F32)
        for group in range(groups):
            ex, ez = group // count_z, group % count_z
            block = vel[comp, pl.ds(ex * 8, 8), pl.ds(ez * 8, 8), :].reshape(64, length_y)
            moved = pltpu.roll(block, (group * 32 + 16) % length_y, 1)
            packed = jnp.where(lane // 32 == group, moved, packed)
        near[index] = packed
    pl.semaphore_wait(barrier, len(greeted))

    def remote(src, dst, ss, rs, where):
        return pltpu.make_async_remote_copy(
            src_ref=src,
            dst_ref=dst,
            send_sem=ss,
            recv_sem=rs,
            device_id=where,
            device_id_type=MESH,
        )

    near_copies = []
    for slot, dx in enumerate((1, -1)):
        copy = remote(near, near_got.at[slot], near_ss.at[slot], near_rs.at[slot], at(dx, 0))
        copy.start()
        near_copies.append(copy)

    for load in loads[1:]:
        load.wait()
    layer_of = lax.broadcasted_iota(jnp.int32, (length_y, count_y), 0) // 8
    layer = lax.broadcasted_iota(jnp.int32, (length_y, count_y), 1)
    height_row = heights[...]
    height = jnp.sum(jnp.where(layer_of == layer, height_row, 0.0), axis=1, keepdims=True)
    lines_mass = height * lines[0]
    lines_hi, lines_lo = split(jnp.concatenate([lines_mass, lines[1] / height], axis=1))
    bound = jnp.max(0.1535 * height_row + 0.000182 / height_row, axis=1, keepdims=True)
    shifts = (0.15 * bound, 0.85 * bound)

    mass_row = jnp.sum(lines_mass, axis=0, keepdims=True)
    scale = columns[0] * mass_row
    for c in range(3):
        field[0, c] = vel[c].reshape(rows, length_y) * scale

    points = owner.shape[1]
    row_x = lagrange_rows(coords[0:1, :])
    row_z = lagrange_rows(coords[1:2, :])
    row_y = lagrange_rows(coords[2:3, :])
    cross = jnp.concatenate([row_x[a : a + 1] * row_z for a in range(8)], axis=0)
    distance = lax.rem(owner[...] - w + n_wall, n_wall)
    from_next = distance == 1
    from_prev = distance == n_wall - 1
    own = jnp.logical_not(jnp.logical_or(from_next, from_prev))
    spread = jnp.concatenate(
        [jnp.where(mask, cross, 0.0) for mask in (own, from_prev, from_next)], axis=0
    )
    n_row = lax.broadcasted_iota(jnp.int32, (length_y, points), 0)
    within = (n_row % 32) // 8
    layer_y = jnp.where(within < NEAR, within + (count_y - NEAR), within - NEAR)
    wanted = (n_row // 32) * count_y + layer_y == element[...]
    along = jnp.where(wanted, jnp.concatenate([row_y] * (length_y // 8), axis=0), 0.0)
    spread = split(spread)

    for copy in near_copies:
        copy.wait()

    sampled = []
    for index in range(2):
        sources = jnp.concatenate(
            [near[index], near_got[0, index], near_got[1, index]], axis=0
        )
        values = dot3(split(sources), spread, TN)
        sampled.append(jnp.sum(values * along, axis=0, keepdims=True))
    stream, spanwise = sampled
    speed = jnp.sqrt(stream * stream + spanwise * spanwise + speed_floor)
    drag = karman / jnp.log(sample_height / roughness[...])
    factor = -(drag * drag * speed / viscosity)
    gradient = (factor * stream, factor * spanwise)
    neumann[0:1, :] = gradient[0]
    neumann[1:2, :] = gradient[1]

    def face_copies(turn):
        copies = []
        for slot, dx in enumerate((1, -1)):
            start = rows - length_z if dx == 1 else 0
            copies.append(
                remote(
                    local.at[turn, :, pl.ds(start, length_z), :],
                    x_got.at[turn, slot],
                    face_ss.at[turn, slot],
                    face_rs.at[turn, slot],
                    at(dx, 0),
                )
            )
        for slot, dz in enumerate((1, -1)):
            copies.append(
                remote(
                    z_send.at[turn, slot],
                    z_got.at[turn, slot],
                    face_ss.at[turn, 2 + slot],
                    face_rs.at[turn, 2 + slot],
                    at(0, dz),
                )
            )
        for slot, (dx, dz) in enumerate(DIRS):
            copies.append(
                remote(
                    c_send.at[turn, slot],
                    c_got.at[turn, slot],
                    face_ss.at[turn, 4 + slot],
                    face_rs.at[turn, 4 + slot],
                    at(dx, dz),
                )
            )
        return copies

    def corner(dx, dz):
        return (rows - length_z if dx == 1 else 0) + (length_z - 1 if dz == 1 else 0)

    def send_faces(turn):
        for c in range(3):
            for slot, dz in enumerate((1, -1)):
                edge = length_z - 1 if dz == 1 else 0
                z_send[turn, slot, c] = local[turn, c, pl.ds(edge, length_x, stride=length_z), :]
            for slot, (dx, dz) in enumerate(DIRS):
                at_row = corner(dx, dz)
                c_send[turn, slot, c : c + 1, :] = local[turn, c, at_row : at_row + 1, :]
        for slot in range(4):
            c_send[turn, slot, 3:8, :] = jnp.zeros((5, length_y), F32)
        copies = face_copies(turn)
        for copy in copies:
            copy.start()
        return copies

    def add_faces(turn, copies):
        for copy in copies:
            copy.wait()
        for c in range(3):
            for slot, dx in enumerate((1, -1)):
                start = 0 if dx == 1 else rows - length_z
                field[turn, c, pl.ds(start, length_z), :] += x_got[turn, slot, c]
            for slot, dz in enumerate((1, -1)):
                edge = pl.ds(0 if dz == 1 else length_z - 1, length_x, stride=length_z)
                field[turn, c, edge, :] = field[turn, c, edge, :] + z_got[turn, slot, c]
            for slot, (dx, dz) in enumerate(DIRS):
                at_row = corner(-dx, -dz)
                field[turn, c, at_row : at_row + 1, :] += c_got[turn, slot, c : c + 1, :]

    def inner(quantity, c, product):
        parts[quantity * 8 + c : quantity * 8 + c + 1, :] = jnp.sum(
            product, axis=0, keepdims=True
        )

    n_line = lax.broadcasted_iota(jnp.int32, (length_y, rows), 0)
    mass_hi = plane_hi[:, rows:]
    mass_lo = plane_lo[:, rows:]
    for index, c in enumerate((0, 2)):
        pull = viscosity * gradient[index]
        lifted = jnp.where(
            n_line == 0, pull[:, :rows], jnp.where(n_line == length_y - 1, pull[:, rows:], 0.0)
        )
        local[0, c] = dot3((mass_hi, mass_lo), split(lifted), NT)
    local[0, 1] = jnp.zeros((rows, length_y), F32)
    copies = send_faces(0)
    parts[...] = jnp.zeros_like(parts)
    for c in (0, 2):
        field[0, c] += local[0, c]
    add_faces(0, copies)

    def operate(source, target):
        for c in range(3):
            lined = dot3(split(field[source, c]), (lines_hi, lines_lo), NN)
            stacked = jnp.concatenate([lined[:, :length_y], lined[:, length_y:]], axis=0)
            local[target, c] = dot3((plane_hi[...], plane_lo[...]), split(stacked), NN)

    slots = {(0, 0): 0, (0, 1): 1, (1, 1): 2, (0, 2): 3, (1, 2): 4, (2, 2): 5}

    def inner_products(newest):
        for c in range(3):
            weighted = field[newest, c] * columns[1]
            for other in range(newest + 1):
                inner(slots[(other, newest)], c, weighted * field[other, c])

    for turn in (1, 2):
        operate(turn - 1, turn)
        copies = send_faces(turn)
        for c in range(3):
            field[turn, c] = local[turn, c] - shifts[turn - 1] * field[turn - 1, c]
        inner_products(turn - 1)
        add_faces(turn, copies)
    operate(2, 3)
    inner_products(2)
    for c in range(3):
        inner(6, c, field[2, c] * columns[2] * local[3, c])

    total_rows = parts.shape[0]
    r_iota = lax.broadcasted_iota(jnp.int32, (total_rows, 128), 0)
    l_iota = lax.broadcasted_iota(jnp.int32, (total_rows, 128), 1)
    diagonal = r_iota == l_iota
    summed = jnp.sum(parts[...], axis=1, keepdims=True)
    row = jnp.sum(jnp.where(diagonal, summed, 0.0), axis=0, keepdims=True)

    def gather_sum(stage, row, count, got, ss, rs, place):
        sum_send[stage] = jnp.broadcast_to(row, (8, 128))
        copies = []
        for k in range(1, count):
            copy = remote(
                sum_send.at[stage], got.at[k - 1], ss.at[k - 1], rs.at[k - 1], place(k)
            )
            copy.start()
            copies.append(copy)
        for copy in copies:
            copy.wait()
        return row + jnp.sum(got[...], axis=0)[0:1]

    if single:
        every = n_wall * n_span
        row = gather_sum(
            0, row, every, wall_got, wall_ss, wall_rs, lambda k: at(k // n_span, k % n_span)
        )
    else:
        row = gather_sum(0, row, n_wall, wall_got, wall_ss, wall_rs, lambda k: at(k, 0))
        row = gather_sum(1, row, n_span, span_got, span_ss, span_rs, lambda k: at(0, k))
    totals = jnp.sum(jnp.where(diagonal, row, 0.0), axis=1, keepdims=True)
    m00, m01, m11, m02, m12, m22, e22 = [totals[q * 8 : q * 8 + 8, :] for q in range(7)]
    t1, t2 = shifts
    a00 = m01 + t1 * m00
    a01 = m11 + t1 * m01
    a02 = m12 + t1 * m02
    a11 = m12 + t2 * m11
    a12 = m22 + t2 * m12
    l10 = a01 / a00
    l20 = a02 / a00
    d1 = a11 - l10 * a01
    u12 = a12 - l10 * a02
    l21 = u12 / d1
    d2 = e22 - l20 * a02 - l21 * u12
    y1 = m01 - l10 * m00
    y2 = m02 - l20 * m00 - l21 * y1
    x2 = y2 / d2
    x1 = y1 / d1 - l21 * x2
    x0 = m00 / a00 - l10 * x1 - l20 * x2
    for c in range(3):
        result = (
            x0[c : c + 1] * field[0, c] + x1[c : c + 1] * field[1, c] + x2[c : c + 1] * field[2, c]
        )
        out[c] = result.reshape(length_x, length_z, length_y)


def body(n_wall, n_span, velocity_old, heights, owner_device, owner_element, ref_coords, roughness):
    sizes = velocity_old.shape[1:]
    length_x, length_z, length_y = sizes
    rows = length_x * length_z
    points = owner_device.shape[0]
    both, lines, columns = tables(*sizes)
    plane_hi, plane_lo = split_np(both)
    every = n_wall * n_span
    first = every if every <= SINGLE_STAGE else n_wall
    vmem = pl.BlockSpec(memory_space=pltpu.VMEM)
    hbm = pl.BlockSpec(memory_space=pltpu.HBM)
    operands = (
        velocity_old,
        heights.reshape(1, -1),
        owner_device.reshape(1, -1),
        owner_element.reshape(1, -1),
        ref_coords,
        roughness.reshape(1, -1),
        plane_hi,
        plane_lo,
        jnp.asarray(lines, F32),
        jnp.asarray(columns, F32),
    )
    dma = pltpu.SemaphoreType.DMA
    return pl.pallas_call(
        functools.partial(kernel, n_wall, n_span, sizes),
        out_shape=(
            jax.ShapeDtypeStruct(velocity_old.shape, F32),
            jax.ShapeDtypeStruct((2, points), F32),
        ),
        in_specs=[hbm] * 10,
        out_specs=(vmem, vmem),
        scratch_shapes=[pltpu.VMEM(value.shape, value.dtype) for value in operands]
        + [
            dma((10,)),
            pltpu.VMEM((2, 64, length_y), F32),
            pltpu.VMEM((2, 2, 64, length_y), F32),
            pltpu.VMEM((3, 3, rows, length_y), F32),
            pltpu.VMEM((4, 3, rows, length_y), F32),
            pltpu.VMEM((ROUNDS, 2, 3, length_x, length_y), F32),
            pltpu.VMEM((ROUNDS, 4, 8, length_y), F32),
            pltpu.VMEM((ROUNDS, 2, 3, length_z, length_y), F32),
            pltpu.VMEM((ROUNDS, 2, 3, length_x, length_y), F32),
            pltpu.VMEM((ROUNDS, 4, 8, length_y), F32),
            pltpu.VMEM((56, length_y), F32),
            pltpu.VMEM((2, 8, 128), F32),
            pltpu.VMEM((first - 1, 8, 128), F32),
            pltpu.VMEM((n_span - 1, 8, 128), F32),
            dma((2,)),
            dma((2,)),
            dma((ROUNDS, 8)),
            dma((ROUNDS, 8)),
            dma((first - 1,)),
            dma((first - 1,)),
            dma((n_span - 1,)),
            dma((n_span - 1,)),
        ],
        compiler_params=pltpu.CompilerParams(
            collective_id=0, has_side_effects=True, vmem_limit_bytes=67043328
        ),
    )(*operands)


def solution(mesh):
    placed = (
        P(None, "wall", "span", None),
        P(),
        P(("wall", "span"), None),
        P(("wall", "span"), None),
        P(None, ("wall", "span")),
        P(("wall", "span")),
    )
    return jax.shard_map(
        functools.partial(body, mesh.shape["wall"], mesh.shape["span"]),
        mesh=mesh,
        in_specs=placed,
        out_specs=(P(None, "wall", "span", None), P(None, ("wall", "span"))),
        check_vma=False,
    )
```

```python
import functools

import jax
import jax.numpy as jnp
import numpy as np
from jax import lax
from jax.experimental import pallas as pl
from jax.experimental.pallas import tpu as pltpu
from jax.sharding import PartitionSpec as P

GLL_NODES = (
    -1.0,
    -0.8717401485096066,
    -0.5917001814331423,
    -0.2092992179024789,
    0.2092992179024789,
    0.5917001814331423,
    0.8717401485096066,
    1.0,
)
GLL_WEIGHTS = (
    0.03571428571428571,
    0.2107042271435061,
    0.3411226924835044,
    0.4124587946587038,
    0.4124587946587038,
    0.3411226924835044,
    0.2107042271435061,
    0.03571428571428571,
)
viscosity = 0.02
inverse_step = 20.0
karman = 0.41
sample_height = 0.1
speed_floor = 0.01
element_dx = 0.05
element_dz = 0.13
NEAR = 2
ROUNDS = 2
REACH = 2
TERMS = (
    (0, 0, 0),
    (1, 1, 2),
    (1, 2, 1),
    (2, 2, 2),
    (3, 3, 6),
    (3, 4, 5),
    (3, 5, 4),
    (3, 6, 3),
    (4, 4, 6),
    (4, 6, 4),
    (5, 5, 6),
    (5, 6, 5),
    (6, 6, 6),
)
SINGLE_STAGE = 64
MESH = pl.DeviceIdType.MESH
F32 = jnp.float32
BF16 = jnp.bfloat16


def stiffness_table():
    points = np.array(GLL_NODES)
    weights = np.array(GLL_WEIGHTS)
    previous = np.ones(8)
    current = points.copy()
    for degree in range(1, 7):
        previous, current = (
            current,
            ((2 * degree + 1) * points * current - degree * previous) / (degree + 1),
        )
    derivative = np.zeros((8, 8))
    for target in range(8):
        for source in range(8):
            if target != source:
                derivative[target, source] = (
                    current[target] / current[source] / (points[target] - points[source])
                )
    derivative[0, 0] = -14.0
    derivative[7, 7] = 14.0
    return derivative.T @ (weights[:, None] * derivative)


def join_matrix(length):
    joined = np.eye(length)
    for left in range(7, length - 1, 8):
        joined[left, left + 1] = 1.0
        joined[left + 1, left] = 1.0
    return joined


def face_weights(length, open_ends):
    values = np.ones(length)
    position = np.arange(length) % 8
    values[(position == 0) | (position == 7)] = 0.5
    if open_ends:
        values[0] = 1.0
        values[-1] = 1.0
    return values


def split_np(matrix):
    single = jnp.asarray(matrix, F32)
    high = single.astype(BF16)
    low = (jnp.asarray(matrix, F32) - high.astype(F32)).astype(BF16)
    return high, low


def tables(length_x, length_z, length_y):
    weights = np.array(GLL_WEIGHTS)
    stiffness = stiffness_table()
    count_x, count_z, count_y = length_x // 8, length_z // 8, length_y // 8
    mass_x = np.tile(0.5 * element_dx * weights, count_x)
    mass_z = np.tile(0.5 * element_dz * weights, count_z)
    stiff_x = np.kron(np.eye(count_x), stiffness * (2.0 / element_dx))
    stiff_z = np.kron(np.eye(count_z), stiffness * (2.0 / element_dz))
    mass_xz = np.kron(mass_x, mass_z)
    join_xz = np.kron(join_matrix(length_x), join_matrix(length_z))
    join_y = join_matrix(length_y)
    plane = viscosity * (
        np.kron(stiff_x, np.diag(mass_z)) + np.kron(np.diag(mass_x), stiff_z)
    ) + inverse_step * np.diag(mass_xz)
    plane = join_xz @ plane
    mass_plane = join_xz @ np.diag(mass_xz)
    both = np.concatenate([plane, mass_plane], axis=1)
    lines_mass = np.tile(0.5 * weights, count_y)[:, None] * join_y
    lines_stiff = viscosity * 2.0 * (np.kron(np.eye(count_y), stiffness) @ join_y)
    lines = np.stack([lines_mass, lines_stiff])
    ring_x = join_matrix(length_x) @ mass_x
    ring_z = join_matrix(length_z) @ mass_z
    ring_x[0] *= 2.0
    ring_x[-1] *= 2.0
    ring_z[0] *= 2.0
    ring_z[-1] *= 2.0
    assembled = inverse_step * np.kron(ring_x, ring_z)
    inner_x = face_weights(length_x, True)
    inner_z = face_weights(length_z, True)
    outer_x = face_weights(length_x, False)
    outer_z = face_weights(length_z, False)
    weight_y = face_weights(length_y, True)
    columns = np.stack(
        [
            assembled[:, None] * np.ones(length_y)[None],
            np.kron(outer_x, outer_z)[:, None] * weight_y[None],
            np.kron(inner_x, inner_z)[:, None] * weight_y[None],
        ]
    )
    reach = 2 * REACH + 1

    def words(length, mass, stiff, extra):
        size = reach * length
        join = join_matrix(size)
        light = join @ np.diag(np.tile(mass, reach))
        heavy = viscosity * join @ np.kron(np.eye(size // 8), stiff) + extra * light
        chains = [
            light,
            heavy @ light,
            light @ light,
            heavy @ heavy @ light,
            heavy @ light @ light,
            light @ heavy @ light,
            light @ light @ light,
        ]
        middle = REACH * length
        chains = [chain[middle : middle + length] for chain in chains]
        return np.concatenate(chains + [np.zeros((128 - 7 * length, size))], axis=0)

    words_x = words(length_x, mass_x, stiffness * (2.0 / element_dx), 0.0)
    words_z = words(length_z, mass_z, stiffness * (2.0 / element_dz), inverse_step)
    pad = np.zeros((128, 128 - reach * length_z))
    words_z = np.concatenate([words_z, pad], axis=1)
    return both, lines, columns, words_x, words_z


def split(value):
    high = value.astype(BF16)
    low = (value - high.astype(F32)).astype(BF16)
    return high, low


def dot3(left, right, dims):
    def one(a, b):
        return lax.dot_general(a, b, (dims, ((), ())), preferred_element_type=F32)

    return one(left[0], right[0]) + (one(left[0], right[1]) + one(left[1], right[0]))


NN = ((1,), (0,))
NT = ((1,), (1,))
TN = ((0,), (0,))
DIRS = ((1, 1), (1, -1), (-1, 1), (-1, -1))


def lagrange_rows(coord):
    points = np.array(GLL_NODES)
    scale = 1.0 / np.prod(points[:, None] - points[None, :] + np.eye(8), axis=1)
    shape = (8, coord.shape[1])
    node = lax.broadcasted_iota(jnp.int32, shape, 0)
    total = jnp.zeros(shape, F32)
    for a in range(8):
        total = jnp.where(node == a, F32(scale[a]), total)
    for b in range(8):
        total = total * jnp.where(node == b, F32(1.0), coord - F32(points[b]))
    return total


def kernel(
    n_wall,
    n_span,
    sizes,
    vel_in,
    heights_in,
    owner_in,
    element_in,
    coords_in,
    roughness_in,
    plane_hi_in,
    plane_lo_in,
    lines_in,
    columns_in,
    words_x_in,
    words_z_in,
    out,
    neumann,
    vel,
    heights,
    owner,
    element,
    coords,
    roughness,
    plane_hi,
    plane_lo,
    lines,
    columns,
    words_x,
    words_z,
    load_sem,
    near,
    near_got,
    field,
    local,
    z_send,
    c_send,
    x_got,
    z_got,
    c_got,
    parts,
    sum_send,
    wall_got,
    span_got,
    pull_send,
    pull_got,
    pull_ss,
    pull_rs,
    near_ss,
    near_rs,
    face_ss,
    face_rs,
    wall_ss,
    wall_rs,
    span_ss,
    span_rs,
):
    length_x, length_z, length_y = sizes
    rows = length_x * length_z
    count_z, count_y = length_z // 8, length_y // 8
    w = lax.axis_index("wall")
    s = lax.axis_index("span")

    def at(dx, dz):
        return (lax.rem(w + (dx + n_wall), n_wall), lax.rem(s + (dz + n_span), n_span))

    loads = [
        pltpu.make_async_copy(source, target, load_sem.at[index])
        for index, (source, target) in enumerate(
            (
                (vel_in, vel),
                (heights_in, heights),
                (lines_in, lines),
                (coords_in, coords),
                (owner_in, owner),
                (element_in, element),
                (columns_in, columns),
                (roughness_in, roughness),
                (plane_hi_in, plane_hi),
                (plane_lo_in, plane_lo),
                (words_x_in, words_x),
                (words_z_in, words_z),
            )
        )
    ]
    for load in loads:
        load.start()

    single = n_wall * n_span <= SINGLE_STAGE
    if single:
        greeted = [divmod(k, n_span) for k in range(1, n_wall * n_span)]
    else:
        greeted = [(k, 0) for k in range(1, n_wall)] + [(0, k) for k in range(1, n_span)]
        greeted += sorted(
            {
                ((dx + n_wall) % n_wall, (dz + n_span) % n_span)
                for dx in range(-REACH, REACH + 1)
                for dz in range(-REACH, REACH + 1)
            }
            - {(0, 0)}
            - set(greeted)
        )
    barrier = pltpu.get_barrier_semaphore()
    for dx, dz in greeted:
        pl.semaphore_signal(barrier, inc=1, device_id=at(dx, dz), device_id_type=MESH)

    loads[0].wait()
    lane = lax.broadcasted_iota(jnp.int32, (64, length_y), 1)
    groups = (length_x // 8) * count_z
    for index, comp in enumerate((0, 2)):
        packed = jnp.zeros((64, length_y), F32)
        for group in range(groups):
            ex, ez = group // count_z, group % count_z
            block = vel[comp, pl.ds(ex * 8, 8), pl.ds(ez * 8, 8), :].reshape(64, length_y)
            moved = pltpu.roll(block, (group * 32 + 16) % length_y, 1)
            packed = jnp.where(lane // 32 == group, moved, packed)
        near[index] = packed
    pl.semaphore_wait(barrier, len(greeted))

    def remote(src, dst, ss, rs, where):
        return pltpu.make_async_remote_copy(
            src_ref=src,
            dst_ref=dst,
            send_sem=ss,
            recv_sem=rs,
            device_id=where,
            device_id_type=MESH,
        )

    near_copies = []
    for slot, dx in enumerate((1, -1)):
        copy = remote(near, near_got.at[slot], near_ss.at[slot], near_rs.at[slot], at(dx, 0))
        copy.start()
        near_copies.append(copy)

    for load in loads[1:]:
        load.wait()
    layer_of = lax.broadcasted_iota(jnp.int32, (length_y, count_y), 0) // 8
    layer = lax.broadcasted_iota(jnp.int32, (length_y, count_y), 1)
    height_row = heights[...]
    height = jnp.sum(jnp.where(layer_of == layer, height_row, 0.0), axis=1, keepdims=True)
    lines_mass = height * lines[0]
    lines_hi, lines_lo = split(jnp.concatenate([lines_mass, lines[1] / height], axis=1))
    bound = jnp.max(0.1535 * height_row + 0.000182 / height_row, axis=1, keepdims=True)
    shifts = (0.15 * bound, 0.85 * bound)

    mass_row = jnp.sum(lines_mass, axis=0, keepdims=True)
    scale = columns[0] * mass_row
    for c in range(3):
        field[0, c] = vel[c].reshape(rows, length_y) * scale

    def face_copies(turn):
        copies = []
        for slot, dx in enumerate((1, -1)):
            start = rows - length_z if dx == 1 else 0
            copies.append(
                remote(
                    local.at[turn, :, pl.ds(start, length_z), :],
                    x_got.at[turn, slot],
                    face_ss.at[turn, slot],
                    face_rs.at[turn, slot],
                    at(dx, 0),
                )
            )
        for slot, dz in enumerate((1, -1)):
            copies.append(
                remote(
                    z_send.at[turn, slot],
                    z_got.at[turn, slot],
                    face_ss.at[turn, 2 + slot],
                    face_rs.at[turn, 2 + slot],
                    at(0, dz),
                )
            )
        for slot, (dx, dz) in enumerate(DIRS):
            copies.append(
                remote(
                    c_send.at[turn, slot],
                    c_got.at[turn, slot],
                    face_ss.at[turn, 4 + slot],
                    face_rs.at[turn, 4 + slot],
                    at(dx, dz),
                )
            )
        return copies

    def corner(dx, dz):
        return (rows - length_z if dx == 1 else 0) + (length_z - 1 if dz == 1 else 0)

    def send_faces(turn):
        for c in range(3):
            for slot, dz in enumerate((1, -1)):
                edge = length_z - 1 if dz == 1 else 0
                z_send[turn, slot, c] = local[turn, c, pl.ds(edge, length_x, stride=length_z), :]
            for slot, (dx, dz) in enumerate(DIRS):
                at_row = corner(dx, dz)
                c_send[turn, slot, c : c + 1, :] = local[turn, c, at_row : at_row + 1, :]
        for slot in range(4):
            c_send[turn, slot, 3:8, :] = jnp.zeros((5, length_y), F32)
        copies = face_copies(turn)
        for copy in copies:
            copy.start()
        return copies

    def add_faces(turn, copies):
        for copy in copies:
            copy.wait()
        for c in range(3):
            for slot, dx in enumerate((1, -1)):
                start = 0 if dx == 1 else rows - length_z
                field[turn + 1, c, pl.ds(start, length_z), :] += x_got[turn, slot, c]
            for slot, dz in enumerate((1, -1)):
                edge = pl.ds(0 if dz == 1 else length_z - 1, length_x, stride=length_z)
                field[turn + 1, c, edge, :] = field[turn + 1, c, edge, :] + z_got[turn, slot, c]
            for slot, (dx, dz) in enumerate(DIRS):
                at_row = corner(-dx, -dz)
                field[turn + 1, c, at_row : at_row + 1, :] += c_got[turn, slot, c : c + 1, :]

    def inner(quantity, c, product):
        parts[quantity * 8 + c : quantity * 8 + c + 1, :] = jnp.sum(
            product, axis=0, keepdims=True
        )

    def operate(source, target):
        for c in range(3):
            lined = dot3(split(field[source, c]), (lines_hi, lines_lo), NN)
            stacked = jnp.concatenate([lined[:, :length_y], lined[:, length_y:]], axis=0)
            local[target, c] = dot3((plane_hi[...], plane_lo[...]), split(stacked), NN)

    slots = {(0, 0): 0, (0, 1): 1, (1, 1): 2, (0, 2): 3, (1, 2): 4, (2, 2): 5}

    def inner_products(newest):
        for c in range(3):
            weighted = field[newest, c] * columns[1]
            for other in range(newest + 1):
                inner(slots[(other, newest)], c, weighted * field[other, c])

    operate(0, 0)
    copies_one = send_faces(0)
    for c in range(3):
        field[1, c] = local[0, c]
    parts[...] = jnp.zeros_like(parts)

    points = owner.shape[1]
    row_x = lagrange_rows(coords[0:1, :])
    row_z = lagrange_rows(coords[1:2, :])
    row_y = lagrange_rows(coords[2:3, :])
    cross = jnp.concatenate([row_x[a : a + 1] * row_z for a in range(8)], axis=0)
    distance = lax.rem(owner[...] - w + n_wall, n_wall)
    from_next = distance == 1
    from_prev = distance == n_wall - 1
    own = jnp.logical_not(jnp.logical_or(from_next, from_prev))
    spread = jnp.concatenate(
        [jnp.where(mask, cross, 0.0) for mask in (own, from_prev, from_next)], axis=0
    )
    n_row = lax.broadcasted_iota(jnp.int32, (length_y, points), 0)
    within = (n_row % 32) // 8
    layer_y = jnp.where(within < NEAR, within + (count_y - NEAR), within - NEAR)
    wanted = (n_row // 32) * count_y + layer_y == element[...]
    along = jnp.where(wanted, jnp.concatenate([row_y] * (length_y // 8), axis=0), 0.0)
    spread = split(spread)

    for copy in near_copies:
        copy.wait()

    sampled = []
    for index in range(2):
        sources = jnp.concatenate(
            [near[index], near_got[0, index], near_got[1, index]], axis=0
        )
        values = dot3(split(sources), spread, TN)
        sampled.append(jnp.sum(values * along, axis=0, keepdims=True))
    stream, spanwise = sampled
    speed = jnp.sqrt(stream * stream + spanwise * spanwise + speed_floor)
    drag = karman / jnp.log(sample_height / roughness[...])
    factor = -(drag * drag * speed / viscosity)
    gradient = (factor * stream, factor * spanwise)
    neumann[0:1, :] = gradient[0]
    neumann[1:2, :] = gradient[1]

    planes = []
    for index in range(2):
        pull = viscosity * gradient[index]
        planes += [pull[:, :rows], pull[:, rows:]]
    node = lax.broadcasted_iota(jnp.int32, (length_x, rows), 1) // length_z
    node_row = lax.broadcasted_iota(jnp.int32, (length_x, rows), 0)
    masked = jnp.concatenate([jnp.where(node == node_row, plane, 0.0) for plane in planes], axis=0)
    pick_row = lax.broadcasted_iota(jnp.int32, (rows, 128), 0)
    pick_lane = lax.broadcasted_iota(jnp.int32, (rows, 128), 1)
    pick = jnp.where(lax.rem(pick_row, length_z) == pick_lane, 1.0, 0.0).astype(BF16)
    masked_hi, masked_lo = split(masked)
    flat = jnp.dot(masked_hi, pick, preferred_element_type=F32) + jnp.dot(
        masked_lo, pick, preferred_element_type=F32
    )
    bundle = flat[0:8]
    tiles = 4 * length_x // 8
    for tile in range(1, tiles):
        bundle = bundle + pltpu.roll(flat[tile * 8 : tile * 8 + 8], tile * length_z, 1)
    pull_send[...] = bundle
    reach = 2 * REACH + 1
    pull_copies = []
    for dx in range(-REACH, REACH + 1):
        for dz in range(-REACH, REACH + 1):
            if (dx, dz) == (0, 0):
                continue
            slot = (REACH - dx) * reach + (REACH - dz)
            copy = remote(
                pull_send, pull_got.at[slot], pull_ss.at[slot], pull_rs.at[slot], at(dx, dz)
            )
            copy.start()
            pull_copies.append(copy)

    add_faces(0, copies_one)
    operate(1, 1)
    copies_two = send_faces(1)
    for c in range(3):
        field[2, c] = local[1, c]
    lines_rows = jnp.concatenate([lines_mass, lines[1] / height], axis=1)
    ends = [lines_rows[0:1], lines_rows[length_y - 1 : length_y]]
    once = [(end[:, :length_y], end[:, length_y:]) for end in ends]
    twice = dot3(
        split(jnp.concatenate([once[0][0], once[0][1], once[1][0], once[1][1]] * 2, axis=0)),
        (lines_hi, lines_lo),
        NN,
    )
    one_lane = lax.broadcasted_iota(jnp.int32, (1, length_y), 1)
    zero = jnp.zeros((1, length_y), F32)
    images = []
    for side in range(2):
        tip = jnp.where(one_lane == side * (length_y - 1), 1.0, 0.0)
        by_mass, by_stiff = twice[2 * side : 2 * side + 1], twice[2 * side + 1 : 2 * side + 2]
        rows_of = [
            (tip, zero, zero),
            (zero, once[side][0], zero),
            (zero, once[side][1], zero),
            (zero, zero, by_mass[:, :length_y]),
            (zero, zero, by_stiff[:, :length_y]),
            (zero, zero, by_mass[:, length_y:]),
            (zero, zero, by_stiff[:, length_y:]),
        ]
        for entry in rows_of:
            image = jnp.concatenate(entry, axis=1)
            images.append(jnp.broadcast_to(image, (length_z, 3 * length_y)))
        images.append(jnp.zeros((128 - 7 * length_z, 3 * length_y), F32))
    images = split(jnp.concatenate(images, axis=0))
    words_x_parts = split(words_x[...])
    words_z_parts = split(words_z[...])

    for copy in pull_copies:
        copy.wait()
    small_lane = lax.broadcasted_iota(jnp.int32, (8, 128), 1) // length_z
    spans = []
    for ix in range(reach):
        pieces = [
            bundle if (ix, iz) == (REACH, REACH) else pull_got[ix * reach + iz]
            for iz in range(reach)
        ]
        for tile in range(tiles):
            line = jnp.zeros((8, 128), F32)
            for iz in range(reach):
                shift = ((iz - tile) * length_z) % 128
                moved = pltpu.roll(pieces[iz], shift, 1) if shift else pieces[iz]
                line = jnp.where(small_lane == iz, moved, line)
            spans.append(line)
    along_z = dot3(split(jnp.concatenate(spans, axis=0)), words_z_parts, NT)
    by_plane = []
    for plane in range(4):
        by_plane.append(
            jnp.concatenate(
                [
                    along_z[(ix * 4 + plane) * length_x : (ix * 4 + plane + 1) * length_x]
                    for ix in range(reach)
                ],
                axis=0,
            )
        )
    both_ways = dot3(words_x_parts, split(jnp.concatenate(by_plane, axis=1)), NN)
    block_lane = lax.broadcasted_iota(jnp.int32, (length_x, 128), 1) // length_z
    keep_row = lax.rem(lax.broadcasted_iota(jnp.int32, (rows, 256), 0), length_z)
    keep_lane = lax.rem(lax.broadcasted_iota(jnp.int32, (rows, 256), 1), length_z)
    tractions = []
    for index in range(2):
        blocks = []
        for side in range(2):
            plane = index * 2 + side
            total = jnp.zeros((length_x, 128), F32)
            for block, word_x, word_z in TERMS:
                piece = both_ways[
                    word_x * length_x : (word_x + 1) * length_x, plane * 128 : plane * 128 + 128
                ]
                shift = ((block - word_z) * length_z) % 128
                moved = pltpu.roll(piece, shift, 1) if shift else piece
                total = total + jnp.where(block_lane == block, moved, 0.0)
            blocks.append(total)
        wide = jnp.concatenate(blocks, axis=1)
        tall = jnp.concatenate(
            [jnp.broadcast_to(wide[x : x + 1], (length_z, 256)) for x in range(length_x)], axis=0
        )
        tall = jnp.where(keep_row == keep_lane, tall, 0.0)
        tractions.append(dot3(split(tall), images, NN))
    add_faces(1, copies_two)
    t1, t2 = shifts
    for c in range(3):
        chain = [field[level, c] for level in range(3)]
        if c != 1:
            taus = tractions[c // 2]
            chain = [
                chain[level] + taus[:, level * length_y : (level + 1) * length_y]
                for level in range(3)
            ]
        v1 = chain[1] - t1 * chain[0]
        field[0, c] = chain[0]
        field[1, c] = v1
        field[2, c] = chain[2] - t1 * chain[1] - t2 * v1
    operate(2, 2)
    for newest in range(3):
        inner_products(newest)
    for c in range(3):
        inner(6, c, field[2, c] * columns[2] * local[2, c])

    total_rows = parts.shape[0]
    r_iota = lax.broadcasted_iota(jnp.int32, (total_rows, 128), 0)
    l_iota = lax.broadcasted_iota(jnp.int32, (total_rows, 128), 1)
    diagonal = r_iota == l_iota
    summed = jnp.sum(parts[...], axis=1, keepdims=True)
    row = jnp.sum(jnp.where(diagonal, summed, 0.0), axis=0, keepdims=True)

    def gather_sum(stage, row, count, got, ss, rs, place):
        sum_send[stage] = jnp.broadcast_to(row, (8, 128))
        copies = []
        for k in range(1, count):
            copy = remote(
                sum_send.at[stage], got.at[k - 1], ss.at[k - 1], rs.at[k - 1], place(k)
            )
            copy.start()
            copies.append(copy)
        for copy in copies:
            copy.wait()
        return row + jnp.sum(got[...], axis=0)[0:1]

    if single:
        every = n_wall * n_span
        row = gather_sum(
            0, row, every, wall_got, wall_ss, wall_rs, lambda k: at(k // n_span, k % n_span)
        )
    else:
        row = gather_sum(0, row, n_wall, wall_got, wall_ss, wall_rs, lambda k: at(k, 0))
        row = gather_sum(1, row, n_span, span_got, span_ss, span_rs, lambda k: at(0, k))
    totals = jnp.sum(jnp.where(diagonal, row, 0.0), axis=1, keepdims=True)
    m00, m01, m11, m02, m12, m22, e22 = [totals[q * 8 : q * 8 + 8, :] for q in range(7)]
    t1, t2 = shifts
    a00 = m01 + t1 * m00
    a01 = m11 + t1 * m01
    a02 = m12 + t1 * m02
    a11 = m12 + t2 * m11
    a12 = m22 + t2 * m12
    l10 = a01 / a00
    l20 = a02 / a00
    d1 = a11 - l10 * a01
    u12 = a12 - l10 * a02
    l21 = u12 / d1
    d2 = e22 - l20 * a02 - l21 * u12
    y1 = m01 - l10 * m00
    y2 = m02 - l20 * m00 - l21 * y1
    x2 = y2 / d2
    x1 = y1 / d1 - l21 * x2
    x0 = m00 / a00 - l10 * x1 - l20 * x2
    for c in range(3):
        result = (
            x0[c : c + 1] * field[0, c] + x1[c : c + 1] * field[1, c] + x2[c : c + 1] * field[2, c]
        )
        out[c] = result.reshape(length_x, length_z, length_y)


def body(n_wall, n_span, velocity_old, heights, owner_device, owner_element, ref_coords, roughness):
    sizes = velocity_old.shape[1:]
    length_x, length_z, length_y = sizes
    rows = length_x * length_z
    points = owner_device.shape[0]
    both, lines, columns, words_x, words_z = tables(*sizes)
    plane_hi, plane_lo = split_np(both)
    every = n_wall * n_span
    first = every if every <= SINGLE_STAGE else n_wall
    vmem = pl.BlockSpec(memory_space=pltpu.VMEM)
    hbm = pl.BlockSpec(memory_space=pltpu.HBM)
    operands = (
        velocity_old,
        heights.reshape(1, -1),
        owner_device.reshape(1, -1),
        owner_element.reshape(1, -1),
        ref_coords,
        roughness.reshape(1, -1),
        plane_hi,
        plane_lo,
        jnp.asarray(lines, F32),
        jnp.asarray(columns, F32),
        jnp.asarray(words_x, F32),
        jnp.asarray(words_z, F32),
    )
    dma = pltpu.SemaphoreType.DMA
    return pl.pallas_call(
        functools.partial(kernel, n_wall, n_span, sizes),
        out_shape=(
            jax.ShapeDtypeStruct(velocity_old.shape, F32),
            jax.ShapeDtypeStruct((2, points), F32),
        ),
        in_specs=[hbm] * 12,
        out_specs=(vmem, vmem),
        scratch_shapes=[pltpu.VMEM(value.shape, value.dtype) for value in operands]
        + [
            dma((12,)),
            pltpu.VMEM((2, 64, length_y), F32),
            pltpu.VMEM((2, 2, 64, length_y), F32),
            pltpu.VMEM((3, 3, rows, length_y), F32),
            pltpu.VMEM((3, 3, rows, length_y), F32),
            pltpu.VMEM((ROUNDS, 2, 3, length_x, length_y), F32),
            pltpu.VMEM((ROUNDS, 4, 8, length_y), F32),
            pltpu.VMEM((ROUNDS, 2, 3, length_z, length_y), F32),
            pltpu.VMEM((ROUNDS, 2, 3, length_x, length_y), F32),
            pltpu.VMEM((ROUNDS, 4, 8, length_y), F32),
            pltpu.VMEM((56, length_y), F32),
            pltpu.VMEM((2, 8, 128), F32),
            pltpu.VMEM((first - 1, 8, 128), F32),
            pltpu.VMEM((n_span - 1, 8, 128), F32),
            pltpu.VMEM((8, 128), F32),
            pltpu.VMEM((25, 8, 128), F32),
            dma((25,)),
            dma((25,)),
            dma((2,)),
            dma((2,)),
            dma((ROUNDS, 8)),
            dma((ROUNDS, 8)),
            dma((first - 1,)),
            dma((first - 1,)),
            dma((n_span - 1,)),
            dma((n_span - 1,)),
        ],
        compiler_params=pltpu.CompilerParams(
            collective_id=0, has_side_effects=True, vmem_limit_bytes=67043328
        ),
    )(*operands)


def solution(mesh):
    placed = (
        P(None, "wall", "span", None),
        P(),
        P(("wall", "span"), None),
        P(("wall", "span"), None),
        P(None, ("wall", "span")),
        P(("wall", "span")),
    )
    return jax.shard_map(
        functools.partial(body, mesh.shape["wall"], mesh.shape["span"]),
        mesh=mesh,
        in_specs=placed,
        out_specs=(P(None, "wall", "span", None), P(None, ("wall", "span"))),
        check_vma=False,
    )
```

```python
import functools

import jax
import jax.numpy as jnp
import numpy as np
from jax import lax
from jax.experimental import pallas as pl
from jax.experimental.pallas import tpu as pltpu
from jax.sharding import PartitionSpec as P

GLL_NODES = (
    -1.0,
    -0.8717401485096066,
    -0.5917001814331423,
    -0.2092992179024789,
    0.2092992179024789,
    0.5917001814331423,
    0.8717401485096066,
    1.0,
)
GLL_WEIGHTS = (
    0.03571428571428571,
    0.2107042271435061,
    0.3411226924835044,
    0.4124587946587038,
    0.4124587946587038,
    0.3411226924835044,
    0.2107042271435061,
    0.03571428571428571,
)
viscosity = 0.02
inverse_step = 20.0
karman = 0.41
sample_height = 0.1
speed_floor = 0.01
element_dx = 0.05
element_dz = 0.13
NEAR = 2
ROUNDS = 2
REACH = 2
TERMS = (
    (0, 0, 0),
    (1, 1, 2),
    (1, 2, 1),
    (2, 2, 2),
    (3, 3, 6),
    (3, 4, 5),
    (3, 5, 4),
    (3, 6, 3),
    (4, 4, 6),
    (4, 6, 4),
    (5, 5, 6),
    (5, 6, 5),
    (6, 6, 6),
)
SINGLE_STAGE = 64
MESH = pl.DeviceIdType.MESH
F32 = jnp.float32
BF16 = jnp.bfloat16


def stiffness_table():
    points = np.array(GLL_NODES)
    weights = np.array(GLL_WEIGHTS)
    previous = np.ones(8)
    current = points.copy()
    for degree in range(1, 7):
        previous, current = (
            current,
            ((2 * degree + 1) * points * current - degree * previous) / (degree + 1),
        )
    derivative = np.zeros((8, 8))
    for target in range(8):
        for source in range(8):
            if target != source:
                derivative[target, source] = (
                    current[target] / current[source] / (points[target] - points[source])
                )
    derivative[0, 0] = -14.0
    derivative[7, 7] = 14.0
    return derivative.T @ (weights[:, None] * derivative)


def join_matrix(length):
    joined = np.eye(length)
    for left in range(7, length - 1, 8):
        joined[left, left + 1] = 1.0
        joined[left + 1, left] = 1.0
    return joined


def face_weights(length, open_ends):
    values = np.ones(length)
    position = np.arange(length) % 8
    values[(position == 0) | (position == 7)] = 0.5
    if open_ends:
        values[0] = 1.0
        values[-1] = 1.0
    return values


def split_np(matrix):
    single = jnp.asarray(matrix, F32)
    high = single.astype(BF16)
    low = (jnp.asarray(matrix, F32) - high.astype(F32)).astype(BF16)
    return high, low


def tables(length_x, length_z, length_y):
    weights = np.array(GLL_WEIGHTS)
    stiffness = stiffness_table()
    count_x, count_z, count_y = length_x // 8, length_z // 8, length_y // 8
    mass_x = np.tile(0.5 * element_dx * weights, count_x)
    mass_z = np.tile(0.5 * element_dz * weights, count_z)
    stiff_x = np.kron(np.eye(count_x), stiffness * (2.0 / element_dx))
    stiff_z = np.kron(np.eye(count_z), stiffness * (2.0 / element_dz))
    mass_xz = np.kron(mass_x, mass_z)
    join_xz = np.kron(join_matrix(length_x), join_matrix(length_z))
    join_y = join_matrix(length_y)
    plane = viscosity * (
        np.kron(stiff_x, np.diag(mass_z)) + np.kron(np.diag(mass_x), stiff_z)
    ) + inverse_step * np.diag(mass_xz)
    plane = join_xz @ plane
    mass_plane = join_xz @ np.diag(mass_xz)
    both = np.concatenate([plane, mass_plane], axis=1)
    lines_mass = np.tile(0.5 * weights, count_y)[:, None] * join_y
    lines_stiff = viscosity * 2.0 * (np.kron(np.eye(count_y), stiffness) @ join_y)
    lines = np.stack([lines_mass, lines_stiff])
    ring_x = join_matrix(length_x) @ mass_x
    ring_z = join_matrix(length_z) @ mass_z
    ring_x[0] *= 2.0
    ring_x[-1] *= 2.0
    ring_z[0] *= 2.0
    ring_z[-1] *= 2.0
    assembled = inverse_step * np.kron(ring_x, ring_z)
    inner_x = face_weights(length_x, True)
    inner_z = face_weights(length_z, True)
    outer_x = face_weights(length_x, False)
    outer_z = face_weights(length_z, False)
    weight_y = face_weights(length_y, True)
    columns = np.stack(
        [
            assembled[:, None] * np.ones(length_y)[None],
            np.kron(outer_x, outer_z)[:, None] * weight_y[None],
            np.kron(inner_x, inner_z)[:, None] * weight_y[None],
        ]
    )
    reach = 2 * REACH + 1

    def words(length, mass, stiff, extra):
        size = reach * length
        join = join_matrix(size)
        light = join @ np.diag(np.tile(mass, reach))
        heavy = viscosity * join @ np.kron(np.eye(size // 8), stiff) + extra * light
        chains = [
            light,
            heavy @ light,
            light @ light,
            heavy @ heavy @ light,
            heavy @ light @ light,
            light @ heavy @ light,
            light @ light @ light,
        ]
        middle = REACH * length
        chains = [chain[middle : middle + length] for chain in chains]
        return np.concatenate(chains + [np.zeros((128 - 7 * length, size))], axis=0)

    words_x = words(length_x, mass_x, stiffness * (2.0 / element_dx), 0.0)
    words_z = words(length_z, mass_z, stiffness * (2.0 / element_dz), inverse_step)
    pad = np.zeros((128, 128 - reach * length_z))
    words_z = np.concatenate([words_z, pad], axis=1)
    return both, lines, columns, words_x, words_z


def split(value):
    high = value.astype(BF16)
    low = (value - high.astype(F32)).astype(BF16)
    return high, low


def dot3(left, right, dims):
    def one(a, b):
        return lax.dot_general(a, b, (dims, ((), ())), preferred_element_type=F32)

    return one(left[0], right[0]) + (one(left[0], right[1]) + one(left[1], right[0]))


NN = ((1,), (0,))
NT = ((1,), (1,))
TN = ((0,), (0,))
DIRS = ((1, 1), (1, -1), (-1, 1), (-1, -1))


def lagrange_rows(coord):
    points = np.array(GLL_NODES)
    scale = 1.0 / np.prod(points[:, None] - points[None, :] + np.eye(8), axis=1)
    shape = (8, coord.shape[1])
    node = lax.broadcasted_iota(jnp.int32, shape, 0)
    total = jnp.zeros(shape, F32)
    for a in range(8):
        total = jnp.where(node == a, F32(scale[a]), total)
    for b in range(8):
        total = total * jnp.where(node == b, F32(1.0), coord - F32(points[b]))
    return total


def kernel(
    n_wall,
    n_span,
    sizes,
    vel_in,
    heights_in,
    owner_in,
    element_in,
    coords_in,
    roughness_in,
    plane_hi_in,
    plane_lo_in,
    lines_in,
    columns_in,
    words_x_in,
    words_z_in,
    out,
    neumann,
    vel,
    heights,
    owner,
    element,
    coords,
    roughness,
    plane_hi,
    plane_lo,
    lines,
    columns,
    words_x,
    words_z,
    load_sem,
    near,
    near_got,
    field,
    local,
    z_send,
    c_send,
    x_got,
    z_got,
    c_got,
    parts,
    sum_send,
    wall_got,
    span_got,
    pull_send,
    pull_got,
    pull_ss,
    pull_rs,
    near_ss,
    near_rs,
    face_ss,
    face_rs,
    wall_ss,
    wall_rs,
    span_ss,
    span_rs,
):
    length_x, length_z, length_y = sizes
    rows = length_x * length_z
    count_z, count_y = length_z // 8, length_y // 8
    w = lax.axis_index("wall")
    s = lax.axis_index("span")

    def at(dx, dz):
        return (lax.rem(w + (dx + n_wall), n_wall), lax.rem(s + (dz + n_span), n_span))

    loads = [
        pltpu.make_async_copy(source, target, load_sem.at[index])
        for index, (source, target) in enumerate(
            (
                (vel_in, vel),
                (heights_in, heights),
                (lines_in, lines),
                (coords_in, coords),
                (owner_in, owner),
                (element_in, element),
                (columns_in, columns),
                (roughness_in, roughness),
                (plane_hi_in, plane_hi),
                (plane_lo_in, plane_lo),
                (words_x_in, words_x),
                (words_z_in, words_z),
            )
        )
    ]
    for load in loads:
        load.start()

    single = n_wall * n_span <= SINGLE_STAGE
    if single:
        greeted = [divmod(k, n_span) for k in range(1, n_wall * n_span)]
    else:
        greeted = [(k, 0) for k in range(1, n_wall)] + [(0, k) for k in range(1, n_span)]
        greeted += sorted(
            {
                ((dx + n_wall) % n_wall, (dz + n_span) % n_span)
                for dx in range(-REACH, REACH + 1)
                for dz in range(-REACH, REACH + 1)
            }
            - {(0, 0)}
            - set(greeted)
        )
    barrier = pltpu.get_barrier_semaphore()
    for dx, dz in greeted:
        pl.semaphore_signal(barrier, inc=1, device_id=at(dx, dz), device_id_type=MESH)

    loads[0].wait()
    lane = lax.broadcasted_iota(jnp.int32, (64, length_y), 1)
    groups = (length_x // 8) * count_z
    for index, comp in enumerate((0, 2)):
        packed = jnp.zeros((64, length_y), F32)
        for group in range(groups):
            ex, ez = group // count_z, group % count_z
            block = vel[comp, pl.ds(ex * 8, 8), pl.ds(ez * 8, 8), :].reshape(64, length_y)
            moved = pltpu.roll(block, (group * 32 + 16) % length_y, 1)
            packed = jnp.where(lane // 32 == group, moved, packed)
        near[index] = packed
    for load in loads[1:]:
        load.wait()

    layer_of = lax.broadcasted_iota(jnp.int32, (length_y, count_y), 0) // 8
    layer = lax.broadcasted_iota(jnp.int32, (length_y, count_y), 1)
    height_row = heights[...]
    height = jnp.sum(jnp.where(layer_of == layer, height_row, 0.0), axis=1, keepdims=True)
    lines_mass = height * lines[0]
    lines_hi, lines_lo = split(jnp.concatenate([lines_mass, lines[1] / height], axis=1))
    bound = jnp.max(0.1535 * height_row + 0.000182 / height_row, axis=1, keepdims=True)
    shifts = (0.15 * bound, 0.85 * bound)

    mass_row = jnp.sum(lines_mass, axis=0, keepdims=True)
    scale = columns[0] * mass_row
    for c in range(3):
        field[0, c] = vel[c].reshape(rows, length_y) * scale

    def remote(src, dst, ss, rs, where):
        return pltpu.make_async_remote_copy(
            src_ref=src,
            dst_ref=dst,
            send_sem=ss,
            recv_sem=rs,
            device_id=where,
            device_id_type=MESH,
        )

    def face_copies(turn):
        copies = []
        for slot, dx in enumerate((1, -1)):
            start = rows - length_z if dx == 1 else 0
            copies.append(
                remote(
                    local.at[turn, :, pl.ds(start, length_z), :],
                    x_got.at[turn, slot],
                    face_ss.at[turn, slot],
                    face_rs.at[turn, slot],
                    at(dx, 0),
                )
            )
        for slot, dz in enumerate((1, -1)):
            copies.append(
                remote(
                    z_send.at[turn, slot],
                    z_got.at[turn, slot],
                    face_ss.at[turn, 2 + slot],
                    face_rs.at[turn, 2 + slot],
                    at(0, dz),
                )
            )
        for slot, (dx, dz) in enumerate(DIRS):
            copies.append(
                remote(
                    c_send.at[turn, slot],
                    c_got.at[turn, slot],
                    face_ss.at[turn, 4 + slot],
                    face_rs.at[turn, 4 + slot],
                    at(dx, dz),
                )
            )
        return copies

    def corner(dx, dz):
        return (rows - length_z if dx == 1 else 0) + (length_z - 1 if dz == 1 else 0)

    def send_faces(turn):
        for c in range(3):
            for slot, dz in enumerate((1, -1)):
                edge = length_z - 1 if dz == 1 else 0
                z_send[turn, slot, c] = local[turn, c, pl.ds(edge, length_x, stride=length_z), :]
            for slot, (dx, dz) in enumerate(DIRS):
                at_row = corner(dx, dz)
                c_send[turn, slot, c : c + 1, :] = local[turn, c, at_row : at_row + 1, :]
        for slot in range(4):
            c_send[turn, slot, 3:8, :] = jnp.zeros((5, length_y), F32)
        if turn == 0:
            pl.semaphore_wait(barrier, len(greeted))
            for copy in near_copies:
                copy.start()
        copies = face_copies(turn)
        for copy in copies:
            copy.start()
        return copies

    def add_faces(turn, copies):
        for copy in copies:
            copy.wait()
        for c in range(3):
            for slot, dx in enumerate((1, -1)):
                start = 0 if dx == 1 else rows - length_z
                field[turn + 1, c, pl.ds(start, length_z), :] += x_got[turn, slot, c]
            for slot, dz in enumerate((1, -1)):
                edge = pl.ds(0 if dz == 1 else length_z - 1, length_x, stride=length_z)
                field[turn + 1, c, edge, :] = field[turn + 1, c, edge, :] + z_got[turn, slot, c]
            for slot, (dx, dz) in enumerate(DIRS):
                at_row = corner(-dx, -dz)
                field[turn + 1, c, at_row : at_row + 1, :] += c_got[turn, slot, c : c + 1, :]

    def inner(quantity, c, product):
        parts[quantity * 8 + c : quantity * 8 + c + 1, :] = jnp.sum(
            product, axis=0, keepdims=True
        )

    def operate(source, target):
        for c in range(3):
            lined = dot3(split(field[source, c]), (lines_hi, lines_lo), NN)
            stacked = jnp.concatenate([lined[:, :length_y], lined[:, length_y:]], axis=0)
            local[target, c] = dot3((plane_hi[...], plane_lo[...]), split(stacked), NN)

    slots = {(0, 0): 0, (0, 1): 1, (1, 1): 2, (0, 2): 3, (1, 2): 4, (2, 2): 5}

    def inner_products(newest):
        for c in range(3):
            weighted = field[newest, c] * columns[1]
            for other in range(newest + 1):
                inner(slots[(other, newest)], c, weighted * field[other, c])

    near_copies = []
    for slot, dx in enumerate((1, -1)):
        copy = remote(near, near_got.at[slot], near_ss.at[slot], near_rs.at[slot], at(dx, 0))
        near_copies.append(copy)

    operate(0, 0)
    copies_one = send_faces(0)
    for c in range(3):
        field[1, c] = local[0, c]
    parts[...] = jnp.zeros_like(parts)

    points = owner.shape[1]
    row_x = lagrange_rows(coords[0:1, :])
    row_z = lagrange_rows(coords[1:2, :])
    row_y = lagrange_rows(coords[2:3, :])
    cross = jnp.concatenate([row_x[a : a + 1] * row_z for a in range(8)], axis=0)
    distance = lax.rem(owner[...] - w + n_wall, n_wall)
    from_next = distance == 1
    from_prev = distance == n_wall - 1
    own = jnp.logical_not(jnp.logical_or(from_next, from_prev))
    spread = jnp.concatenate(
        [jnp.where(mask, cross, 0.0) for mask in (own, from_prev, from_next)], axis=0
    )
    n_row = lax.broadcasted_iota(jnp.int32, (length_y, points), 0)
    within = (n_row % 32) // 8
    layer_y = jnp.where(within < NEAR, within + (count_y - NEAR), within - NEAR)
    wanted = (n_row // 32) * count_y + layer_y == element[...]
    along = jnp.where(wanted, jnp.concatenate([row_y] * (length_y // 8), axis=0), 0.0)
    spread = split(spread)

    for copy in near_copies:
        copy.wait()

    sampled = []
    for index in range(2):
        sources = jnp.concatenate(
            [near[index], near_got[0, index], near_got[1, index]], axis=0
        )
        values = dot3(split(sources), spread, TN)
        sampled.append(jnp.sum(values * along, axis=0, keepdims=True))
    stream, spanwise = sampled
    speed = jnp.sqrt(stream * stream + spanwise * spanwise + speed_floor)
    drag = karman / jnp.log(sample_height / roughness[...])
    factor = -(drag * drag * speed / viscosity)
    gradient = (factor * stream, factor * spanwise)
    neumann[0:1, :] = gradient[0]
    neumann[1:2, :] = gradient[1]

    planes = []
    for index in range(2):
        pull = viscosity * gradient[index]
        planes += [pull[:, :rows], pull[:, rows:]]
    node = lax.broadcasted_iota(jnp.int32, (length_x, rows), 1) // length_z
    node_row = lax.broadcasted_iota(jnp.int32, (length_x, rows), 0)
    masked = jnp.concatenate([jnp.where(node == node_row, plane, 0.0) for plane in planes], axis=0)
    pick_row = lax.broadcasted_iota(jnp.int32, (rows, 128), 0)
    pick_lane = lax.broadcasted_iota(jnp.int32, (rows, 128), 1)
    pick = jnp.where(lax.rem(pick_row, length_z) == pick_lane, 1.0, 0.0).astype(BF16)
    masked_hi, masked_lo = split(masked)
    flat = jnp.dot(masked_hi, pick, preferred_element_type=F32) + jnp.dot(
        masked_lo, pick, preferred_element_type=F32
    )
    bundle = flat[0:8]
    tiles = 4 * length_x // 8
    for tile in range(1, tiles):
        bundle = bundle + pltpu.roll(flat[tile * 8 : tile * 8 + 8], tile * length_z, 1)
    pull_send[...] = bundle
    reach = 2 * REACH + 1
    folded = n_span == 2 * REACH
    pull_copies = []
    for dx in range(-REACH, REACH + 1):
        for dz in range(-REACH, REACH + 1):
            if (dx, dz) == (0, 0) or (folded and dz == REACH):
                continue
            slot = (REACH - dx) * reach + (REACH - dz)
            copy = remote(
                pull_send, pull_got.at[slot], pull_ss.at[slot], pull_rs.at[slot], at(dx, dz)
            )
            copy.start()
            pull_copies.append(copy)

    add_faces(0, copies_one)
    operate(1, 1)
    copies_two = send_faces(1)
    for c in range(3):
        field[2, c] = local[1, c]
    lines_rows = jnp.concatenate([lines_mass, lines[1] / height], axis=1)
    ends = [lines_rows[0:1], lines_rows[length_y - 1 : length_y]]
    once = [(end[:, :length_y], end[:, length_y:]) for end in ends]
    twice = dot3(
        split(jnp.concatenate([once[0][0], once[0][1], once[1][0], once[1][1]] * 2, axis=0)),
        (lines_hi, lines_lo),
        NN,
    )
    one_lane = lax.broadcasted_iota(jnp.int32, (1, length_y), 1)
    zero = jnp.zeros((1, length_y), F32)
    images = []
    for side in range(2):
        tip = jnp.where(one_lane == side * (length_y - 1), 1.0, 0.0)
        by_mass, by_stiff = twice[2 * side : 2 * side + 1], twice[2 * side + 1 : 2 * side + 2]
        rows_of = [
            (tip, zero, zero),
            (zero, once[side][0], zero),
            (zero, once[side][1], zero),
            (zero, zero, by_mass[:, :length_y]),
            (zero, zero, by_stiff[:, :length_y]),
            (zero, zero, by_mass[:, length_y:]),
            (zero, zero, by_stiff[:, length_y:]),
        ]
        for entry in rows_of:
            image = jnp.concatenate(entry, axis=1)
            images.append(jnp.broadcast_to(image, (length_z, 3 * length_y)))
        images.append(jnp.zeros((128 - 7 * length_z, 3 * length_y), F32))
    images = split(jnp.concatenate(images, axis=0))
    words_x_parts = split(words_x[...])
    words_z_parts = split(words_z[...])

    for copy in pull_copies:
        copy.wait()
    small_lane = lax.broadcasted_iota(jnp.int32, (8, 128), 1) // length_z
    spans = []
    for ix in range(reach):
        pieces = [
            bundle
            if (ix, iz) == (REACH, REACH)
            else pull_got[ix * reach + (reach - 1 if folded and iz == 0 else iz)]
            for iz in range(reach)
        ]
        for tile in range(tiles):
            line = jnp.zeros((8, 128), F32)
            for iz in range(reach):
                shift = ((iz - tile) * length_z) % 128
                moved = pltpu.roll(pieces[iz], shift, 1) if shift else pieces[iz]
                line = jnp.where(small_lane == iz, moved, line)
            spans.append(line)
    along_z = dot3(split(jnp.concatenate(spans, axis=0)), words_z_parts, NT)
    by_plane = []
    for plane in range(4):
        by_plane.append(
            jnp.concatenate(
                [
                    along_z[(ix * 4 + plane) * length_x : (ix * 4 + plane + 1) * length_x]
                    for ix in range(reach)
                ],
                axis=0,
            )
        )
    both_ways = dot3(words_x_parts, split(jnp.concatenate(by_plane, axis=1)), NN)
    block_lane = lax.broadcasted_iota(jnp.int32, (length_x, 128), 1) // length_z
    keep_row = lax.rem(lax.broadcasted_iota(jnp.int32, (rows, 256), 0), length_z)
    keep_lane = lax.rem(lax.broadcasted_iota(jnp.int32, (rows, 256), 1), length_z)
    tractions = []
    for index in range(2):
        blocks = []
        for side in range(2):
            plane = index * 2 + side
            total = jnp.zeros((length_x, 128), F32)
            for block, word_x, word_z in TERMS:
                piece = both_ways[
                    word_x * length_x : (word_x + 1) * length_x, plane * 128 : plane * 128 + 128
                ]
                shift = ((block - word_z) * length_z) % 128
                moved = pltpu.roll(piece, shift, 1) if shift else piece
                total = total + jnp.where(block_lane == block, moved, 0.0)
            blocks.append(total)
        wide = jnp.concatenate(blocks, axis=1)
        tall = jnp.concatenate(
            [jnp.broadcast_to(wide[x : x + 1], (length_z, 256)) for x in range(length_x)], axis=0
        )
        tall = jnp.where(keep_row == keep_lane, tall, 0.0)
        tractions.append(dot3(split(tall), images, NN))
    add_faces(1, copies_two)
    t1, t2 = shifts
    for c in range(3):
        chain = [field[level, c] for level in range(3)]
        if c != 1:
            taus = tractions[c // 2]
            chain = [
                chain[level] + taus[:, level * length_y : (level + 1) * length_y]
                for level in range(3)
            ]
        v1 = chain[1] - t1 * chain[0]
        field[0, c] = chain[0]
        field[1, c] = v1
        field[2, c] = chain[2] - t1 * chain[1] - t2 * v1
    operate(2, 2)
    for newest in range(3):
        inner_products(newest)
    for c in range(3):
        inner(6, c, field[2, c] * columns[2] * local[2, c])

    total_rows = parts.shape[0]
    r_iota = lax.broadcasted_iota(jnp.int32, (total_rows, 128), 0)
    l_iota = lax.broadcasted_iota(jnp.int32, (total_rows, 128), 1)
    diagonal = r_iota == l_iota
    summed = jnp.sum(parts[...], axis=1, keepdims=True)
    row = jnp.sum(jnp.where(diagonal, summed, 0.0), axis=0, keepdims=True)

    def gather_sum(stage, row, count, got, ss, rs, place):
        sum_send[stage : stage + 1, :] = row
        copies = []
        for k in range(1, count):
            copy = remote(
                sum_send.at[pl.ds(stage, 1), :],
                got.at[pl.ds(k - 1, 1), :],
                ss.at[k - 1],
                rs.at[k - 1],
                place(k),
            )
            copy.start()
            copies.append(copy)
        for copy in copies:
            copy.wait()
        return row + jnp.sum(got[...], axis=0, keepdims=True)

    if single:
        every = n_wall * n_span
        row = gather_sum(
            0, row, every, wall_got, wall_ss, wall_rs, lambda k: at(k // n_span, k % n_span)
        )
    else:
        row = gather_sum(0, row, n_wall, wall_got, wall_ss, wall_rs, lambda k: at(k, 0))
        row = gather_sum(1, row, n_span, span_got, span_ss, span_rs, lambda k: at(0, k))
    totals = jnp.sum(jnp.where(diagonal, row, 0.0), axis=1, keepdims=True)
    m00, m01, m11, m02, m12, m22, e22 = [totals[q * 8 : q * 8 + 8, :] for q in range(7)]
    t1, t2 = shifts
    a00 = m01 + t1 * m00
    a01 = m11 + t1 * m01
    a02 = m12 + t1 * m02
    a11 = m12 + t2 * m11
    a12 = m22 + t2 * m12
    l10 = a01 / a00
    l20 = a02 / a00
    d1 = a11 - l10 * a01
    u12 = a12 - l10 * a02
    l21 = u12 / d1
    d2 = e22 - l20 * a02 - l21 * u12
    y1 = m01 - l10 * m00
    y2 = m02 - l20 * m00 - l21 * y1
    x2 = y2 / d2
    x1 = y1 / d1 - l21 * x2
    x0 = m00 / a00 - l10 * x1 - l20 * x2
    for c in range(3):
        result = (
            x0[c : c + 1] * field[0, c] + x1[c : c + 1] * field[1, c] + x2[c : c + 1] * field[2, c]
        )
        out[c] = result.reshape(length_x, length_z, length_y)


def body(n_wall, n_span, velocity_old, heights, owner_device, owner_element, ref_coords, roughness):
    sizes = velocity_old.shape[1:]
    length_x, length_z, length_y = sizes
    rows = length_x * length_z
    points = owner_device.shape[0]
    both, lines, columns, words_x, words_z = tables(*sizes)
    plane_hi, plane_lo = split_np(both)
    every = n_wall * n_span
    first = every if every <= SINGLE_STAGE else n_wall
    vmem = pl.BlockSpec(memory_space=pltpu.VMEM)
    hbm = pl.BlockSpec(memory_space=pltpu.HBM)
    operands = (
        velocity_old,
        heights.reshape(1, -1),
        owner_device.reshape(1, -1),
        owner_element.reshape(1, -1),
        ref_coords,
        roughness.reshape(1, -1),
        plane_hi,
        plane_lo,
        jnp.asarray(lines, F32),
        jnp.asarray(columns, F32),
        jnp.asarray(words_x, F32),
        jnp.asarray(words_z, F32),
    )
    dma = pltpu.SemaphoreType.DMA
    return pl.pallas_call(
        functools.partial(kernel, n_wall, n_span, sizes),
        out_shape=(
            jax.ShapeDtypeStruct(velocity_old.shape, F32),
            jax.ShapeDtypeStruct((2, points), F32),
        ),
        in_specs=[hbm] * 12,
        out_specs=(vmem, vmem),
        scratch_shapes=[pltpu.VMEM(value.shape, value.dtype) for value in operands]
        + [
            dma((12,)),
            pltpu.VMEM((2, 64, length_y), F32),
            pltpu.VMEM((2, 2, 64, length_y), F32),
            pltpu.VMEM((3, 3, rows, length_y), F32),
            pltpu.VMEM((3, 3, rows, length_y), F32),
            pltpu.VMEM((ROUNDS, 2, 3, length_x, length_y), F32),
            pltpu.VMEM((ROUNDS, 4, 8, length_y), F32),
            pltpu.VMEM((ROUNDS, 2, 3, length_z, length_y), F32),
            pltpu.VMEM((ROUNDS, 2, 3, length_x, length_y), F32),
            pltpu.VMEM((ROUNDS, 4, 8, length_y), F32),
            pltpu.VMEM((56, length_y), F32),
            pltpu.VMEM((2, 128), F32),
            pltpu.VMEM((first - 1, 128), F32),
            pltpu.VMEM((n_span - 1, 128), F32),
            pltpu.VMEM((8, 128), F32),
            pltpu.VMEM((25, 8, 128), F32),
            dma((25,)),
            dma((25,)),
            dma((2,)),
            dma((2,)),
            dma((ROUNDS, 8)),
            dma((ROUNDS, 8)),
            dma((first - 1,)),
            dma((first - 1,)),
            dma((n_span - 1,)),
            dma((n_span - 1,)),
        ],
        compiler_params=pltpu.CompilerParams(
            collective_id=0, has_side_effects=True, vmem_limit_bytes=67043328
        ),
    )(*operands)


def solution(mesh):
    placed = (
        P(None, "wall", "span", None),
        P(),
        P(("wall", "span"), None),
        P(("wall", "span"), None),
        P(None, ("wall", "span")),
        P(("wall", "span")),
    )
    return jax.shard_map(
        functools.partial(body, mesh.shape["wall"], mesh.shape["span"]),
        mesh=mesh,
        in_specs=placed,
        out_specs=(P(None, "wall", "span", None), P(None, ("wall", "span"))),
        check_vma=False,
    )
```

```python
import functools

import jax
import jax.numpy as jnp
import numpy as np
from jax import lax
from jax.experimental import pallas as pl
from jax.experimental.pallas import tpu as pltpu
from jax.sharding import PartitionSpec as P

GLL_NODES = (
    -1.0,
    -0.8717401485096066,
    -0.5917001814331423,
    -0.2092992179024789,
    0.2092992179024789,
    0.5917001814331423,
    0.8717401485096066,
    1.0,
)
GLL_WEIGHTS = (
    0.03571428571428571,
    0.2107042271435061,
    0.3411226924835044,
    0.4124587946587038,
    0.4124587946587038,
    0.3411226924835044,
    0.2107042271435061,
    0.03571428571428571,
)
viscosity = 0.02
inverse_step = 20.0
karman = 0.41
sample_height = 0.1
speed_floor = 0.01
element_dx = 0.05
element_dz = 0.13
NEAR = 2
ROUNDS = 2
REACH = 2
TERMS = (
    (0, 0, 0),
    (1, 1, 2),
    (1, 2, 1),
    (2, 2, 2),
    (3, 3, 6),
    (3, 4, 5),
    (3, 5, 4),
    (3, 6, 3),
    (4, 4, 6),
    (4, 6, 4),
    (5, 5, 6),
    (5, 6, 5),
    (6, 6, 6),
)
SINGLE_STAGE = 64
MESH = pl.DeviceIdType.MESH
F32 = jnp.float32
BF16 = jnp.bfloat16


def stiffness_table():
    points = np.array(GLL_NODES)
    weights = np.array(GLL_WEIGHTS)
    previous = np.ones(8)
    current = points.copy()
    for degree in range(1, 7):
        previous, current = (
            current,
            ((2 * degree + 1) * points * current - degree * previous) / (degree + 1),
        )
    derivative = np.zeros((8, 8))
    for target in range(8):
        for source in range(8):
            if target != source:
                derivative[target, source] = (
                    current[target] / current[source] / (points[target] - points[source])
                )
    derivative[0, 0] = -14.0
    derivative[7, 7] = 14.0
    return derivative.T @ (weights[:, None] * derivative)


def join_matrix(length):
    joined = np.eye(length)
    for left in range(7, length - 1, 8):
        joined[left, left + 1] = 1.0
        joined[left + 1, left] = 1.0
    return joined


def face_weights(length, open_ends):
    values = np.ones(length)
    position = np.arange(length) % 8
    values[(position == 0) | (position == 7)] = 0.5
    if open_ends:
        values[0] = 1.0
        values[-1] = 1.0
    return values


def split_np(matrix):
    single = jnp.asarray(matrix, F32)
    high = single.astype(BF16)
    low = (jnp.asarray(matrix, F32) - high.astype(F32)).astype(BF16)
    return high, low


def tables(length_x, length_z, length_y):
    weights = np.array(GLL_WEIGHTS)
    stiffness = stiffness_table()
    count_x, count_z, count_y = length_x // 8, length_z // 8, length_y // 8
    mass_x = np.tile(0.5 * element_dx * weights, count_x)
    mass_z = np.tile(0.5 * element_dz * weights, count_z)
    stiff_x = np.kron(np.eye(count_x), stiffness * (2.0 / element_dx))
    stiff_z = np.kron(np.eye(count_z), stiffness * (2.0 / element_dz))
    mass_xz = np.kron(mass_x, mass_z)
    join_xz = np.kron(join_matrix(length_x), join_matrix(length_z))
    join_y = join_matrix(length_y)
    plane = viscosity * (
        np.kron(stiff_x, np.diag(mass_z)) + np.kron(np.diag(mass_x), stiff_z)
    ) + inverse_step * np.diag(mass_xz)
    plane = join_xz @ plane
    mass_plane = join_xz @ np.diag(mass_xz)
    both = np.concatenate([plane, mass_plane], axis=1)
    lines_mass = np.tile(0.5 * weights, count_y)[:, None] * join_y
    lines_stiff = viscosity * 2.0 * (np.kron(np.eye(count_y), stiffness) @ join_y)
    lines = np.stack([lines_mass, lines_stiff])
    ring_x = join_matrix(length_x) @ mass_x
    ring_z = join_matrix(length_z) @ mass_z
    ring_x[0] *= 2.0
    ring_x[-1] *= 2.0
    ring_z[0] *= 2.0
    ring_z[-1] *= 2.0
    assembled = inverse_step * np.kron(ring_x, ring_z)
    inner_x = face_weights(length_x, True)
    inner_z = face_weights(length_z, True)
    outer_x = face_weights(length_x, False)
    outer_z = face_weights(length_z, False)
    weight_y = face_weights(length_y, True)
    columns = np.stack(
        [
            assembled[:, None] * np.ones(length_y)[None],
            np.kron(outer_x, outer_z)[:, None] * weight_y[None],
            np.kron(inner_x, inner_z)[:, None] * weight_y[None],
        ]
    )
    reach = 2 * REACH + 1

    def words(length, mass, stiff, extra):
        size = reach * length
        join = join_matrix(size)
        light = join @ np.diag(np.tile(mass, reach))
        heavy = viscosity * join @ np.kron(np.eye(size // 8), stiff) + extra * light
        chains = [
            light,
            heavy @ light,
            light @ light,
            heavy @ heavy @ light,
            heavy @ light @ light,
            light @ heavy @ light,
            light @ light @ light,
        ]
        middle = REACH * length
        chains = [chain[middle : middle + length] for chain in chains]
        return np.concatenate(chains + [np.zeros((128 - 7 * length, size))], axis=0)

    words_x = words(length_x, mass_x, stiffness * (2.0 / element_dx), 0.0)
    words_z = words(length_z, mass_z, stiffness * (2.0 / element_dz), inverse_step)
    pad = np.zeros((128, 128 - reach * length_z))
    words_z = np.concatenate([words_z, pad], axis=1)
    return both, lines, columns, words_x, words_z


def split(value):
    high = value.astype(BF16)
    low = (value - high.astype(F32)).astype(BF16)
    return high, low


def dot3(left, right, dims):
    def one(a, b):
        return lax.dot_general(a, b, (dims, ((), ())), preferred_element_type=F32)

    return one(left[0], right[0]) + (one(left[0], right[1]) + one(left[1], right[0]))


NN = ((1,), (0,))
NT = ((1,), (1,))
TN = ((0,), (0,))
DIRS = ((1, 1), (1, -1), (-1, 1), (-1, -1))


def lagrange_rows(coord):
    points = np.array(GLL_NODES)
    scale = 1.0 / np.prod(points[:, None] - points[None, :] + np.eye(8), axis=1)
    shape = (8, coord.shape[1])
    node = lax.broadcasted_iota(jnp.int32, shape, 0)
    total = jnp.zeros(shape, F32)
    for a in range(8):
        total = jnp.where(node == a, F32(scale[a]), total)
    for b in range(8):
        total = total * jnp.where(node == b, F32(1.0), coord - F32(points[b]))
    return total


def kernel(
    n_wall,
    n_span,
    sizes,
    vel_in,
    heights_in,
    owner_in,
    element_in,
    coords_in,
    roughness_in,
    plane_hi_in,
    plane_lo_in,
    lines_in,
    columns_in,
    words_x_in,
    words_z_in,
    out,
    neumann,
    vel,
    heights,
    owner,
    element,
    coords,
    roughness,
    plane_hi,
    plane_lo,
    lines,
    columns,
    words_x,
    words_z,
    load_sem,
    near,
    near_got,
    field,
    local,
    z_send,
    c_send,
    x_got,
    z_got,
    c_got,
    parts,
    sum_send,
    wall_got,
    span_got,
    pull_send,
    pull_got,
    pull_ss,
    pull_rs,
    near_ss,
    near_rs,
    face_ss,
    face_rs,
    wall_ss,
    wall_rs,
    span_ss,
    span_rs,
):
    length_x, length_z, length_y = sizes
    rows = length_x * length_z
    count_z, count_y = length_z // 8, length_y // 8
    w = lax.axis_index("wall")
    s = lax.axis_index("span")

    def at(dx, dz):
        return (lax.rem(w + (dx + n_wall), n_wall), lax.rem(s + (dz + n_span), n_span))

    loads = [
        pltpu.make_async_copy(source, target, load_sem.at[index])
        for index, (source, target) in enumerate(
            (
                (vel_in, vel),
                (heights_in, heights),
                (lines_in, lines),
                (coords_in, coords),
                (owner_in, owner),
                (element_in, element),
                (columns_in, columns),
                (roughness_in, roughness),
                (plane_hi_in, plane_hi),
                (plane_lo_in, plane_lo),
                (words_x_in, words_x),
                (words_z_in, words_z),
            )
        )
    ]
    for load in loads:
        load.start()

    single = n_wall * n_span <= SINGLE_STAGE
    if single:
        greeted = [divmod(k, n_span) for k in range(1, n_wall * n_span)]
    else:
        greeted = [(k, 0) for k in range(1, n_wall)] + [(0, k) for k in range(1, n_span)]
        greeted += sorted(
            {
                ((dx + n_wall) % n_wall, (dz + n_span) % n_span)
                for dx in range(-REACH, REACH + 1)
                for dz in range(-REACH, REACH + 1)
            }
            - {(0, 0)}
            - set(greeted)
        )
    barrier = pltpu.get_barrier_semaphore()
    for dx, dz in greeted:
        pl.semaphore_signal(barrier, inc=1, device_id=at(dx, dz), device_id_type=MESH)

    loads[0].wait()
    lane = lax.broadcasted_iota(jnp.int32, (64, length_y), 1)
    groups = (length_x // 8) * count_z
    for index, comp in enumerate((0, 2)):
        packed = jnp.zeros((64, length_y), F32)
        for group in range(groups):
            ex, ez = group // count_z, group % count_z
            block = vel[comp, pl.ds(ex * 8, 8), pl.ds(ez * 8, 8), :].reshape(64, length_y)
            moved = pltpu.roll(block, (group * 32 + 16) % length_y, 1)
            packed = jnp.where(lane // 32 == group, moved, packed)
        near[index] = packed
    for load in loads[1:]:
        load.wait()

    layer_of = lax.broadcasted_iota(jnp.int32, (length_y, count_y), 0) // 8
    layer = lax.broadcasted_iota(jnp.int32, (length_y, count_y), 1)
    height_row = heights[...]
    height = jnp.sum(jnp.where(layer_of == layer, height_row, 0.0), axis=1, keepdims=True)
    lines_mass = height * lines[0]
    lines_hi, lines_lo = split(jnp.concatenate([lines_mass, lines[1] / height], axis=1))
    bound = jnp.max(0.1535 * height_row + 0.000182 / height_row, axis=1, keepdims=True)
    shifts = (0.15 * bound, 0.85 * bound)

    mass_row = jnp.sum(lines_mass, axis=0, keepdims=True)
    scale = columns[0] * mass_row
    for c in range(3):
        field[0, c] = vel[c].reshape(rows, length_y) * scale

    def remote(src, dst, ss, rs, where):
        return pltpu.make_async_remote_copy(
            src_ref=src,
            dst_ref=dst,
            send_sem=ss,
            recv_sem=rs,
            device_id=where,
            device_id_type=MESH,
        )

    def face_copies(turn):
        copies = []
        for slot, dx in enumerate((1, -1)):
            start = rows - length_z if dx == 1 else 0
            copies.append(
                remote(
                    local.at[turn, :, pl.ds(start, length_z), :],
                    x_got.at[turn, slot],
                    face_ss.at[turn, slot],
                    face_rs.at[turn, slot],
                    at(dx, 0),
                )
            )
        for slot, dz in enumerate((1, -1)):
            copies.append(
                remote(
                    z_send.at[turn, slot],
                    z_got.at[turn, slot],
                    face_ss.at[turn, 2 + slot],
                    face_rs.at[turn, 2 + slot],
                    at(0, dz),
                )
            )
        for slot, (dx, dz) in enumerate(DIRS):
            copies.append(
                remote(
                    c_send.at[turn, slot, pl.ds(0, 3), :],
                    c_got.at[turn, slot, pl.ds(0, 3), :],
                    face_ss.at[turn, 4 + slot],
                    face_rs.at[turn, 4 + slot],
                    at(dx, dz),
                )
            )
        return copies

    def corner(dx, dz):
        return (rows - length_z if dx == 1 else 0) + (length_z - 1 if dz == 1 else 0)

    def send_faces(turn):
        for c in range(3):
            for slot, dz in enumerate((1, -1)):
                edge = length_z - 1 if dz == 1 else 0
                z_send[turn, slot, c] = local[turn, c, pl.ds(edge, length_x, stride=length_z), :]
            for slot, (dx, dz) in enumerate(DIRS):
                at_row = corner(dx, dz)
                c_send[turn, slot, c : c + 1, :] = local[turn, c, at_row : at_row + 1, :]
        if turn == 0:
            pl.semaphore_wait(barrier, len(greeted))
            for copy in near_copies:
                copy.start()
        copies = face_copies(turn)
        for copy in copies:
            copy.start()
        return copies

    def add_faces(turn, copies):
        for copy in copies:
            copy.wait()
        for c in range(3):
            for slot, dx in enumerate((1, -1)):
                start = 0 if dx == 1 else rows - length_z
                field[turn + 1, c, pl.ds(start, length_z), :] += x_got[turn, slot, c]
            for slot, dz in enumerate((1, -1)):
                edge = pl.ds(0 if dz == 1 else length_z - 1, length_x, stride=length_z)
                field[turn + 1, c, edge, :] = field[turn + 1, c, edge, :] + z_got[turn, slot, c]
            for slot, (dx, dz) in enumerate(DIRS):
                at_row = corner(-dx, -dz)
                field[turn + 1, c, at_row : at_row + 1, :] += c_got[turn, slot, c : c + 1, :]

    def inner(quantity, c, product):
        parts[quantity * 8 + c : quantity * 8 + c + 1, :] = jnp.sum(
            product, axis=0, keepdims=True
        )

    def operate(source, target):
        flat = field[source].reshape(3 * rows, length_y)
        lined = dot3(split(flat), (lines_hi, lines_lo), NN)
        wide = jnp.concatenate(
            [
                jnp.concatenate(
                    [
                        lined[c * rows : (c + 1) * rows, :length_y],
                        lined[c * rows : (c + 1) * rows, length_y:],
                    ],
                    axis=0,
                )
                for c in range(3)
            ],
            axis=1,
        )
        result = dot3((plane_hi[...], plane_lo[...]), split(wide), NN)
        for c in range(3):
            local[target, c] = result[:, c * length_y : (c + 1) * length_y]

    slots = {(0, 0): 0, (0, 1): 1, (1, 1): 2, (0, 2): 3, (1, 2): 4, (2, 2): 5}

    def inner_products(newest):
        for c in range(3):
            weighted = field[newest, c] * columns[1]
            for other in range(newest + 1):
                inner(slots[(other, newest)], c, weighted * field[other, c])

    near_copies = []
    for slot, dx in enumerate((1, -1)):
        copy = remote(near, near_got.at[slot], near_ss.at[slot], near_rs.at[slot], at(dx, 0))
        near_copies.append(copy)

    operate(0, 0)
    copies_one = send_faces(0)
    for c in range(3):
        field[1, c] = local[0, c]
    parts[...] = jnp.zeros_like(parts)

    points = owner.shape[1]
    row_x = lagrange_rows(coords[0:1, :])
    row_z = lagrange_rows(coords[1:2, :])
    row_y = lagrange_rows(coords[2:3, :])
    cross = jnp.concatenate([row_x[a : a + 1] * row_z for a in range(8)], axis=0)
    distance = lax.rem(owner[...] - w + n_wall, n_wall)
    from_next = distance == 1
    from_prev = distance == n_wall - 1
    own = jnp.logical_not(jnp.logical_or(from_next, from_prev))
    spread = jnp.concatenate(
        [jnp.where(mask, cross, 0.0) for mask in (own, from_prev, from_next)], axis=0
    )
    n_row = lax.broadcasted_iota(jnp.int32, (length_y, points), 0)
    within = (n_row % 32) // 8
    layer_y = jnp.where(within < NEAR, within + (count_y - NEAR), within - NEAR)
    wanted = (n_row // 32) * count_y + layer_y == element[...]
    along = jnp.where(wanted, jnp.concatenate([row_y] * (length_y // 8), axis=0), 0.0)
    spread = split(spread)

    for copy in near_copies:
        copy.wait()

    sampled = []
    for index in range(2):
        sources = jnp.concatenate(
            [near[index], near_got[0, index], near_got[1, index]], axis=0
        )
        values = dot3(split(sources), spread, TN)
        sampled.append(jnp.sum(values * along, axis=0, keepdims=True))
    stream, spanwise = sampled
    speed = jnp.sqrt(stream * stream + spanwise * spanwise + speed_floor)
    drag = karman / jnp.log(sample_height / roughness[...])
    factor = -(drag * drag * speed / viscosity)
    gradient = (factor * stream, factor * spanwise)
    neumann[0:1, :] = gradient[0]
    neumann[1:2, :] = gradient[1]

    planes = []
    for index in range(2):
        pull = viscosity * gradient[index]
        planes += [pull[:, :rows], pull[:, rows:]]
    node = lax.broadcasted_iota(jnp.int32, (length_x, rows), 1) // length_z
    node_row = lax.broadcasted_iota(jnp.int32, (length_x, rows), 0)
    masked = jnp.concatenate([jnp.where(node == node_row, plane, 0.0) for plane in planes], axis=0)
    pick_row = lax.broadcasted_iota(jnp.int32, (rows, 128), 0)
    pick_lane = lax.broadcasted_iota(jnp.int32, (rows, 128), 1)
    pick = jnp.where(lax.rem(pick_row, length_z) == pick_lane, 1.0, 0.0).astype(BF16)
    masked_hi, masked_lo = split(masked)
    flat = jnp.dot(masked_hi, pick, preferred_element_type=F32) + jnp.dot(
        masked_lo, pick, preferred_element_type=F32
    )
    bundle = flat[0:8]
    tiles = 4 * length_x // 8
    for tile in range(1, tiles):
        bundle = bundle + pltpu.roll(flat[tile * 8 : tile * 8 + 8], tile * length_z, 1)
    pull_send[...] = bundle
    reach = 2 * REACH + 1
    folded = n_span == 2 * REACH
    pull_copies = []
    offsets = [
        (dx, dz)
        for dx in range(-REACH, REACH + 1)
        for dz in range(-REACH, REACH + 1)
        if (dx, dz) != (0, 0) and not (folded and dz == REACH)
    ]
    for dx, dz in sorted(offsets, key=lambda pair: -abs(pair[0]) - abs(pair[1])):
        slot = (REACH - dx) * reach + (REACH - dz)
        copy = remote(
            pull_send, pull_got.at[slot], pull_ss.at[slot], pull_rs.at[slot], at(dx, dz)
        )
        copy.start()
        pull_copies.append(copy)

    add_faces(0, copies_one)
    operate(1, 1)
    copies_two = send_faces(1)
    for c in range(3):
        field[2, c] = local[1, c]
    lines_rows = jnp.concatenate([lines_mass, lines[1] / height], axis=1)
    ends = [lines_rows[0:1], lines_rows[length_y - 1 : length_y]]
    once = [(end[:, :length_y], end[:, length_y:]) for end in ends]
    twice = dot3(
        split(jnp.concatenate([once[0][0], once[0][1], once[1][0], once[1][1]] * 2, axis=0)),
        (lines_hi, lines_lo),
        NN,
    )
    one_lane = lax.broadcasted_iota(jnp.int32, (1, length_y), 1)
    zero = jnp.zeros((1, length_y), F32)
    images = []
    for side in range(2):
        tip = jnp.where(one_lane == side * (length_y - 1), 1.0, 0.0)
        by_mass, by_stiff = twice[2 * side : 2 * side + 1], twice[2 * side + 1 : 2 * side + 2]
        rows_of = [
            (tip, zero, zero),
            (zero, once[side][0], zero),
            (zero, once[side][1], zero),
            (zero, zero, by_mass[:, :length_y]),
            (zero, zero, by_stiff[:, :length_y]),
            (zero, zero, by_mass[:, length_y:]),
            (zero, zero, by_stiff[:, length_y:]),
        ]
        for entry in rows_of:
            image = jnp.concatenate(entry, axis=1)
            images.append(jnp.broadcast_to(image, (length_z, 3 * length_y)))
        images.append(jnp.zeros((128 - 7 * length_z, 3 * length_y), F32))
    images = split(jnp.concatenate(images, axis=0))
    words_x_parts = split(words_x[...])
    words_z_parts = split(words_z[...])

    for copy in pull_copies:
        copy.wait()
    small_lane = lax.broadcasted_iota(jnp.int32, (8, 128), 1) // length_z
    spans = []
    for ix in range(reach):
        pieces = [
            bundle
            if (ix, iz) == (REACH, REACH)
            else pull_got[ix * reach + (reach - 1 if folded and iz == 0 else iz)]
            for iz in range(reach)
        ]
        for tile in range(tiles):
            line = jnp.zeros((8, 128), F32)
            for iz in range(reach):
                shift = ((iz - tile) * length_z) % 128
                moved = pltpu.roll(pieces[iz], shift, 1) if shift else pieces[iz]
                line = jnp.where(small_lane == iz, moved, line)
            spans.append(line)
    along_z = dot3(split(jnp.concatenate(spans, axis=0)), words_z_parts, NT)
    by_plane = []
    for plane in range(4):
        by_plane.append(
            jnp.concatenate(
                [
                    along_z[(ix * 4 + plane) * length_x : (ix * 4 + plane + 1) * length_x]
                    for ix in range(reach)
                ],
                axis=0,
            )
        )
    both_ways = dot3(words_x_parts, split(jnp.concatenate(by_plane, axis=1)), NN)
    block_lane = lax.broadcasted_iota(jnp.int32, (length_x, 128), 1) // length_z
    keep_row = lax.rem(lax.broadcasted_iota(jnp.int32, (rows, 256), 0), length_z)
    keep_lane = lax.rem(lax.broadcasted_iota(jnp.int32, (rows, 256), 1), length_z)
    tractions = []
    for index in range(2):
        blocks = []
        for side in range(2):
            plane = index * 2 + side
            total = jnp.zeros((length_x, 128), F32)
            for block, word_x, word_z in TERMS:
                piece = both_ways[
                    word_x * length_x : (word_x + 1) * length_x, plane * 128 : plane * 128 + 128
                ]
                shift = ((block - word_z) * length_z) % 128
                moved = pltpu.roll(piece, shift, 1) if shift else piece
                total = total + jnp.where(block_lane == block, moved, 0.0)
            blocks.append(total)
        wide = jnp.concatenate(blocks, axis=1)
        tall = jnp.concatenate(
            [jnp.broadcast_to(wide[x : x + 1], (length_z, 256)) for x in range(length_x)], axis=0
        )
        tall = jnp.where(keep_row == keep_lane, tall, 0.0)
        tractions.append(dot3(split(tall), images, NN))
    add_faces(1, copies_two)
    t1, t2 = shifts
    for c in range(3):
        chain = [field[level, c] for level in range(3)]
        if c != 1:
            taus = tractions[c // 2]
            chain = [
                chain[level] + taus[:, level * length_y : (level + 1) * length_y]
                for level in range(3)
            ]
        v1 = chain[1] - t1 * chain[0]
        field[0, c] = chain[0]
        field[1, c] = v1
        field[2, c] = chain[2] - t1 * chain[1] - t2 * v1
    operate(2, 2)
    for newest in range(3):
        inner_products(newest)
    for c in range(3):
        inner(6, c, field[2, c] * columns[2] * local[2, c])

    total_rows = parts.shape[0]
    r_iota = lax.broadcasted_iota(jnp.int32, (total_rows, 128), 0)
    l_iota = lax.broadcasted_iota(jnp.int32, (total_rows, 128), 1)
    diagonal = r_iota == l_iota
    summed = jnp.sum(parts[...], axis=1, keepdims=True)
    row = jnp.sum(jnp.where(diagonal, summed, 0.0), axis=0, keepdims=True)

    def gather_sum(stage, row, count, got, ss, rs, place):
        sum_send[stage : stage + 1, :] = row
        copies = []
        for k in range(1, count):
            copy = remote(
                sum_send.at[pl.ds(stage, 1), :],
                got.at[pl.ds(k - 1, 1), :],
                ss.at[k - 1],
                rs.at[k - 1],
                place(k),
            )
            copy.start()
            copies.append(copy)
        for copy in copies:
            copy.wait()
        return row + jnp.sum(got[...], axis=0, keepdims=True)

    if single:
        every = n_wall * n_span
        row = gather_sum(
            0, row, every, wall_got, wall_ss, wall_rs, lambda k: at(k // n_span, k % n_span)
        )
    else:
        row = gather_sum(0, row, n_wall, wall_got, wall_ss, wall_rs, lambda k: at(k, 0))
        row = gather_sum(1, row, n_span, span_got, span_ss, span_rs, lambda k: at(0, k))
    totals = jnp.sum(jnp.where(diagonal, row, 0.0), axis=1, keepdims=True)
    m00, m01, m11, m02, m12, m22, e22 = [totals[q * 8 : q * 8 + 8, :] for q in range(7)]
    t1, t2 = shifts
    a00 = m01 + t1 * m00
    a01 = m11 + t1 * m01
    a02 = m12 + t1 * m02
    a11 = m12 + t2 * m11
    a12 = m22 + t2 * m12
    l10 = a01 / a00
    l20 = a02 / a00
    d1 = a11 - l10 * a01
    u12 = a12 - l10 * a02
    l21 = u12 / d1
    d2 = e22 - l20 * a02 - l21 * u12
    y1 = m01 - l10 * m00
    y2 = m02 - l20 * m00 - l21 * y1
    x2 = y2 / d2
    x1 = y1 / d1 - l21 * x2
    x0 = m00 / a00 - l10 * x1 - l20 * x2
    for c in range(3):
        result = (
            x0[c : c + 1] * field[0, c] + x1[c : c + 1] * field[1, c] + x2[c : c + 1] * field[2, c]
        )
        out[c] = result.reshape(length_x, length_z, length_y)


def body(n_wall, n_span, velocity_old, heights, owner_device, owner_element, ref_coords, roughness):
    sizes = velocity_old.shape[1:]
    length_x, length_z, length_y = sizes
    rows = length_x * length_z
    points = owner_device.shape[0]
    both, lines, columns, words_x, words_z = tables(*sizes)
    plane_hi, plane_lo = split_np(both)
    every = n_wall * n_span
    first = every if every <= SINGLE_STAGE else n_wall
    vmem = pl.BlockSpec(memory_space=pltpu.VMEM)
    hbm = pl.BlockSpec(memory_space=pltpu.HBM)
    operands = (
        velocity_old,
        heights.reshape(1, -1),
        owner_device.reshape(1, -1),
        owner_element.reshape(1, -1),
        ref_coords,
        roughness.reshape(1, -1),
        plane_hi,
        plane_lo,
        jnp.asarray(lines, F32),
        jnp.asarray(columns, F32),
        jnp.asarray(words_x, F32),
        jnp.asarray(words_z, F32),
    )
    dma = pltpu.SemaphoreType.DMA
    return pl.pallas_call(
        functools.partial(kernel, n_wall, n_span, sizes),
        out_shape=(
            jax.ShapeDtypeStruct(velocity_old.shape, F32),
            jax.ShapeDtypeStruct((2, points), F32),
        ),
        in_specs=[hbm] * 12,
        out_specs=(vmem, vmem),
        scratch_shapes=[pltpu.VMEM(value.shape, value.dtype) for value in operands]
        + [
            dma((12,)),
            pltpu.VMEM((2, 64, length_y), F32),
            pltpu.VMEM((2, 2, 64, length_y), F32),
            pltpu.VMEM((3, 3, rows, length_y), F32),
            pltpu.VMEM((3, 3, rows, length_y), F32),
            pltpu.VMEM((ROUNDS, 2, 3, length_x, length_y), F32),
            pltpu.VMEM((ROUNDS, 4, 8, length_y), F32),
            pltpu.VMEM((ROUNDS, 2, 3, length_z, length_y), F32),
            pltpu.VMEM((ROUNDS, 2, 3, length_x, length_y), F32),
            pltpu.VMEM((ROUNDS, 4, 8, length_y), F32),
            pltpu.VMEM((56, length_y), F32),
            pltpu.VMEM((2, 128), F32),
            pltpu.VMEM((first - 1, 128), F32),
            pltpu.VMEM((n_span - 1, 128), F32),
            pltpu.VMEM((8, 128), F32),
            pltpu.VMEM((25, 8, 128), F32),
            dma((25,)),
            dma((25,)),
            dma((2,)),
            dma((2,)),
            dma((ROUNDS, 8)),
            dma((ROUNDS, 8)),
            dma((first - 1,)),
            dma((first - 1,)),
            dma((n_span - 1,)),
            dma((n_span - 1,)),
        ],
        compiler_params=pltpu.CompilerParams(
            collective_id=0, has_side_effects=True, vmem_limit_bytes=67043328
        ),
    )(*operands)


def solution(mesh):
    placed = (
        P(None, "wall", "span", None),
        P(),
        P(("wall", "span"), None),
        P(("wall", "span"), None),
        P(None, ("wall", "span")),
        P(("wall", "span")),
    )
    return jax.shard_map(
        functools.partial(body, mesh.shape["wall"], mesh.shape["span"]),
        mesh=mesh,
        in_specs=placed,
        out_specs=(P(None, "wall", "span", None), P(None, ("wall", "span"))),
        check_vma=False,
    )
```
